32 devices in a mesh: dp: 8 (over z, core), tensor: 4 (over y, x).
Axes of the slice: x: 2, y: 2, z: 4, core: 2. Of those that a mesh axis runs over, the one named last changes fastest.
Arguments:
- inputs: bfloat16 [8192, 2048], P(('dp', 'tensor'))
- doc_lengths: int32 [8, 4], P('dp'), may hold values from 0 to 1024, as said below
- attn_gain: bfloat16 [2048], P('dp'), may hold values from 0.099609375 to 1.8984375
- w_query: bfloat16 [2048, 2048], P('dp', 'tensor')
- w_key: bfloat16 [2048, 512], P('dp', 'tensor')
- value_weight: bfloat16 [2048, 512], P('dp', 'tensor'), may hold values from -0.125 to 0.125
- w_output: bfloat16 [2048, 2048], P('tensor', 'dp'), may hold values from -0.5 to 0.5
- mlp_gain: bfloat16 [2048], P('dp'), may hold values from 0.099609375 to 1.8984375
- w_gate: bfloat16 [2048, 8192], P('dp', 'tensor'), may hold values from -0.125 to 0.125
- w_up: bfloat16 [2048, 8192], P('dp', 'tensor'), may hold values from -0.125 to 0.125
- w_down: bfloat16 [8192, 2048], P('tensor', 'dp'), may hold values from -0.125 to 0.125
- out_grad: bfloat16 [8192, 2048], P(('dp', 'tensor')), may hold values from -6 to 6
Outputs:
- output: float32 [8192, 2048], P(('dp', 'tensor'))
- input_grad: float32 [8192, 2048], P(('dp', 'tensor'))
- attn_gain_grad: float32 [2048], P('dp')
- w_query_grad: float32 [2048, 2048], P('dp', 'tensor')
- w_key_grad: float32 [2048, 512], P('dp', 'tensor')
- w_value_grad: float32 [2048, 512], P('dp', 'tensor')
- w_output_grad: float32 [2048, 2048], P('tensor', 'dp')
- mlp_gain_grad: float32 [2048], P('dp')
- w_gate_grad: float32 [2048, 8192], P('dp', 'tensor')
- w_up_grad: float32 [2048, 8192], P('dp', 'tensor')
- w_down_grad: float32 [8192, 2048], P('tensor', 'dp')
The draws below stay inside these ranges and needn't reach their ends.
Inputs may be any that keep to these rules, and one draw needn't show every extreme that they name: `doc_lengths`: row r lists the lengths of the 4 documents packed back to back from the first slot of dp index r; a row sums to at most 1024, zero lengths occur, and in every draw some row holds a single document of 1024 tokens.
All inputs are finite; a program needn't handle non-finite values.
Results may differ from the reference program's by a relative error of at most 0.017.
The reference program's roundings to bfloat16 on the way count: a program that leaves them out, or rounds other values in their place, can miss the bound.
Values may be sent and summed in bfloat16 or wider, within the bound.
A program may use at most 256 MiB of HBM per device.

```python
import math
import jax
import jax.numpy as jnp
from jax import lax

MODEL_WIDTH = 2048
HQ = 32
KEY_VALUE_HEADS = 8
HEAD_SIZE = 64
FF = 8192
ROWS = 1024
DOCS = 4
QBLK = 512
TOKENS = 8192
N_DP = 8


def draw_inputs(key, part):
    key_rows, key_cols, key_main = jax.random.split(key, 3)
    row_scale = jnp.exp(jax.random.uniform(key_rows, (TOKENS, 1), jnp.float32, math.log(0.4), math.log(4.0)))
    column_scale = jnp.exp(jax.random.uniform(key_cols, (1, MODEL_WIDTH), jnp.float32, math.log(0.3), math.log(3.0)))
    primary_portion = jax.random.normal(key_main, (TOKENS, MODEL_WIDTH), jnp.float32)
    return jnp.clip(primary_portion * row_scale * column_scale, -16.0, 16.0).astype(jnp.bfloat16)


def draw_doc_lengths(key, part):
    key_full, key_fill, key_cuts = jax.random.split(key, 3)
    full_row = jax.random.randint(key_full, (), 0, N_DP)
    fills = jax.random.randint(key_fill, (N_DP,), ROWS // 4, ROWS + 1)
    cuts = jnp.sort(jax.random.randint(key_cuts, (N_DP, DOCS - 1), 0, ROWS + 1), axis=1)
    bounds = jnp.concatenate([jnp.zeros((N_DP, 1), jnp.int32), cuts * fills[:, None] // ROWS, fills[:, None]], axis=1)
    lengths = bounds[:, 1:] - bounds[:, :-1]
    single = jnp.where(jnp.arange(DOCS) == 0, ROWS, 0).astype(jnp.int32)
    chosen = (jnp.arange(N_DP) == full_row)[:, None]
    return jnp.where(chosen, single[None, :], lengths).astype(jnp.int32)


def draw_w_query(key, part):
    key_main = jax.random.fold_in(key, 0)
    primary_portion = jnp.clip(jax.random.normal(key_main, (MODEL_WIDTH, HQ * HEAD_SIZE), jnp.float32), -6.0, 6.0) * MODEL_WIDTH ** (-0.5)
    head_scale = jnp.ones((HQ,), jnp.float32)
    return (primary_portion * jnp.repeat(head_scale, HEAD_SIZE)[None, :]).astype(jnp.bfloat16)


def draw_w_key(key, part):
    primary_portion = jnp.clip(jax.random.normal(key, (MODEL_WIDTH, KEY_VALUE_HEADS * HEAD_SIZE), jnp.float32), -6.0, 6.0) * MODEL_WIDTH ** (-0.5)
    return primary_portion.astype(jnp.bfloat16)


def shard_levels(stream_key, dims, shards, low, high):
    def one(axis_at, parts):
        draws = jax.random.uniform(jax.random.fold_in(jax.random.fold_in(stream_key, 6), axis_at), (parts,), jnp.float32, low / len(shards), high / len(shards))
        return jnp.repeat(jnp.exp(draws), dims[axis_at] // parts).reshape((-1,) + (1,) * (len(dims) - axis_at - 1))

    loudness = one(*shards[0])
    for cut in shards[1:]:
        loudness = loudness * one(*cut)
    return loudness


def scatter_about(key, extent, width, limit, cuts=(), kind=jnp.bfloat16):
    level = shard_levels(key, extent, cuts, -0.22, 0.18) if cuts else 1.0
    drawn = jax.random.normal(key, extent, jnp.float32) * width * level
    return jnp.minimum(jnp.maximum(drawn, -limit), limit).astype(kind)


def setup_inputs(seed: int = 0) -> dict:
    streams_of = jax.random.split(jax.random.key(seed), 13)
    return {
        "inputs": draw_inputs(jax.random.fold_in(streams_of[12], 71), 0),
        "doc_lengths": draw_doc_lengths(jax.random.fold_in(streams_of[12], 71), 0),
        "attn_gain": jnp.clip(1.0 + 0.18 * jax.random.normal(streams_of[2], (MODEL_WIDTH,), jnp.float32), 0.099609375, 1.8984375).astype(jnp.bfloat16),
        "w_query": draw_w_query(jax.random.fold_in(streams_of[12], 71), 0),
        "w_key": draw_w_key(jax.random.fold_in(streams_of[12], 71), 0),
        "value_weight": scatter_about(streams_of[5], (MODEL_WIDTH, KEY_VALUE_HEADS * HEAD_SIZE), MODEL_WIDTH ** -0.5, 0.125, ((0, 8), (1, 4))),
        "w_output": scatter_about(streams_of[6], (HQ * HEAD_SIZE, MODEL_WIDTH), (HQ * HEAD_SIZE // 16) ** -0.5, 0.5, ((0, 4), (1, 8))),
        "mlp_gain": jnp.clip(1.0 + 0.18 * jax.random.normal(streams_of[7], (MODEL_WIDTH,), jnp.float32), 0.099609375, 1.8984375).astype(jnp.bfloat16),
        "w_gate": scatter_about(streams_of[8], (MODEL_WIDTH, FF), MODEL_WIDTH ** -0.5, 0.125, ((0, 8), (1, 4))),
        "w_up": scatter_about(streams_of[9], (MODEL_WIDTH, FF), MODEL_WIDTH ** -0.5, 0.125, ((0, 8), (1, 4))),
        "w_down": scatter_about(streams_of[10], (FF, MODEL_WIDTH), (FF // 4) ** -0.5, 0.125, ((0, 4), (1, 8))),
        "out_grad": scatter_about(streams_of[11], (TOKENS, MODEL_WIDTH), 1.0, 6.0, ((0, 32),)),
    }


epsilon = 1e-05
rope_base = 500000.0

def layout(lengths, total_rows):
    row_index = jnp.arange(total_rows, dtype=jnp.int32)
    doc_ends = jnp.cumsum(lengths).astype(jnp.int32)
    passed = doc_ends[None, :] <= row_index[:, None]
    document_segment = lax.optimization_barrier(jnp.sum(passed.astype(jnp.int32), axis=1)).astype(jnp.int32)
    doc_start = lax.optimization_barrier(jnp.sum(jnp.where(passed, lengths[None, :], 0), axis=1)).astype(jnp.int32)
    positions = (row_index - doc_start).astype(jnp.float32)
    valid_rows = (document_segment < lengths.shape[0]).astype(jnp.float32)
    return (document_segment, positions, valid_rows)

def rope_tables(positions, head_dim):
    half_dim = head_dim // 2
    inverse_freq = rope_base ** (-(jnp.arange(half_dim, dtype=jnp.float32) * 2.0 / head_dim))
    angles = positions[:, None] * inverse_freq[None, :]
    return (jnp.cos(angles)[:, None, :], jnp.sin(angles)[:, None, :])

def rotate(tensor, cosine, sine_part, direction):
    half_dim = tensor.shape[-1] // 2
    first_half = tensor[..., :half_dim]
    second_half = tensor[..., half_dim:]
    return jnp.concatenate([first_half * cosine - direction * second_half * sine_part, second_half * cosine + direction * first_half * sine_part], axis=-1)

def rms_stats(hidden):
    scale_row = lax.rsqrt(lax.optimization_barrier(jnp.mean(hidden * hidden, axis=-1, keepdims=True)) + epsilon)
    return (scale_row, hidden * scale_row)

def norm_backward(grad_normed, unit_rows, scale_row, gain_wide):
    scaled = grad_normed * gain_wide
    return scale_row * (scaled - unit_rows * lax.optimization_barrier(jnp.mean(scaled * unit_rows, axis=-1, keepdims=True)))

def rounded(tensor):
    return lax.optimization_barrier(tensor.astype(jnp.bfloat16)).astype(jnp.float32)

def block_mask(document_segment, first_row, block_rows):
    row_index = jnp.arange(document_segment.shape[0], dtype=jnp.int32)
    query_rows = first_row + jnp.arange(block_rows, dtype=jnp.int32)
    query_segment = lax.dynamic_slice_in_dim(document_segment, first_row, block_rows, 0)
    return (query_segment[:, None] == document_segment[None, :]) & (row_index[None, :] <= query_rows[:, None])

def attention_forward(queries, keys_rot, values, document_segment, block_rows):
    total_rows, kv_heads, group_size, head_dim = queries.shape
    score_scale = head_dim ** (-0.5)
    keys_wide = keys_rot.astype(jnp.float32)
    values_wide = values.astype(jnp.float32)

    def one_block(block_index):
        first_row = (block_index * block_rows).astype(jnp.int32)
        query_block = lax.dynamic_slice_in_dim(queries, first_row, block_rows, 0).astype(jnp.float32)
        allowed = block_mask(document_segment, first_row, block_rows)
        scores = jnp.einsum('qkgd,skd->kgqs', query_block, keys_wide) * score_scale
        scores = jnp.where(allowed, scores, -jnp.inf)
        row_max = lax.optimization_barrier(jnp.max(scores, axis=-1, keepdims=True))
        log_total = row_max + jnp.log(lax.optimization_barrier(jnp.sum(jnp.exp(scores - row_max), axis=-1, keepdims=True)))
        weights = rounded(jnp.exp(scores - log_total))
        attended = jnp.einsum('kgqs,skd->qkgd', weights, values_wide)
        return (attended.astype(jnp.bfloat16), log_total[..., 0])
    attended, log_total = lax.map(one_block, jnp.arange(total_rows // block_rows, dtype=jnp.int32))
    return (attended.reshape(total_rows, kv_heads, group_size, head_dim), log_total)

def attention_backward(queries, keys_rot, values, attended, grad_attended, log_total, document_segment, block_rows):
    total_rows, kv_heads, group_size, head_dim = queries.shape
    score_scale = head_dim ** (-0.5)
    keys_wide = keys_rot.astype(jnp.float32)
    values_wide = values.astype(jnp.float32)

    def one_block(running, block_index):
        key_grad, value_grad = running
        first_row = (block_index * block_rows).astype(jnp.int32)
        query_block = lax.dynamic_slice_in_dim(queries, first_row, block_rows, 0).astype(jnp.float32)
        block_gradient = lax.dynamic_slice_in_dim(grad_attended, first_row, block_rows, 0).astype(jnp.float32)
        out_block = lax.dynamic_slice_in_dim(attended, first_row, block_rows, 0).astype(jnp.float32)
        allowed = block_mask(document_segment, first_row, block_rows)
        scores = jnp.einsum('qkgd,skd->kgqs', query_block, keys_wide) * score_scale
        scores = jnp.where(allowed, scores, -jnp.inf)
        prob_full = jnp.exp(scores - log_total[block_index][..., None])
        weights = rounded(prob_full)
        value_grad = value_grad + jnp.einsum('kgqs,qkgd->skd', weights, block_gradient)
        grad_probs = jnp.einsum('qkgd,skd->kgqs', block_gradient, values_wide)
        row_delta = jnp.einsum('qkgd,qkgd->kgq', block_gradient, out_block)
        grad_scores = rounded(prob_full * (grad_probs - row_delta[..., None]))
        query_grad = jnp.einsum('kgqs,skd->qkgd', grad_scores, keys_wide) * score_scale
        key_grad = key_grad + jnp.einsum('kgqs,qkgd->skd', grad_scores, query_block) * score_scale
        return ((key_grad, value_grad), query_grad)
    zero_keys = jnp.zeros((total_rows, kv_heads, head_dim), jnp.float32)
    (key_grad, value_grad), query_grad = lax.scan(one_block, (zero_keys, zero_keys), jnp.arange(total_rows // block_rows, dtype=jnp.int32))
    return (query_grad.reshape(total_rows, kv_heads * group_size, head_dim), key_grad, value_grad)

def layer_group(inputs, lengths, out_grad, params):
    attn_gain, w_query, w_key, value_weight, w_output, mlp_gain, w_gate, w_up, w_down = params
    total_rows = inputs.shape[0]
    head_count = w_query.shape[1] // HEAD_SIZE
    kv_heads = w_key.shape[1] // HEAD_SIZE
    group_size = head_count // kv_heads
    document_segment, positions, valid_rows = layout(lengths, total_rows)
    valid_col = valid_rows[:, None]
    cosine, sine_part = rope_tables(positions, HEAD_SIZE)
    gain_one = attn_gain.astype(jnp.float32)
    gain_two = mlp_gain.astype(jnp.float32)
    residual = inputs.astype(jnp.float32)
    scale_one, unit_one = rms_stats(residual)
    normed_one = (unit_one * gain_one).astype(jnp.bfloat16)
    query_full = jnp.dot(normed_one, w_query, preferred_element_type=jnp.float32).reshape(total_rows, head_count, HEAD_SIZE)
    queries = rotate(query_full, cosine, sine_part, 1.0).astype(jnp.bfloat16).reshape(total_rows, kv_heads, group_size, HEAD_SIZE)
    key_full = jnp.dot(normed_one, w_key, preferred_element_type=jnp.float32).reshape(total_rows, kv_heads, HEAD_SIZE)
    keys_rot = rotate(key_full, cosine, sine_part, 1.0).astype(jnp.bfloat16)
    values = jnp.dot(normed_one, value_weight, preferred_element_type=jnp.float32).astype(jnp.bfloat16).reshape(total_rows, kv_heads, HEAD_SIZE)
    attended, log_total = attention_forward(queries, keys_rot, values, document_segment, QBLK)
    attended_flat = attended.reshape(total_rows, head_count * HEAD_SIZE)
    hidden = residual + valid_col * jnp.dot(attended_flat, w_output, preferred_element_type=jnp.float32)
    scale_two, unit_two = rms_stats(hidden)
    normed_two = (unit_two * gain_two).astype(jnp.bfloat16)
    gate_pre = jnp.dot(normed_two, w_gate, preferred_element_type=jnp.float32)
    up_proj = jnp.dot(normed_two, w_up, preferred_element_type=jnp.float32)
    sigmoid_gate = jax.nn.sigmoid(gate_pre)
    activation = (gate_pre * sigmoid_gate * up_proj).astype(jnp.bfloat16)
    output = hidden + valid_col * jnp.dot(activation, w_down, preferred_element_type=jnp.float32)
    grad_out = out_grad.astype(jnp.float32)
    grad_mlp = (grad_out * valid_col).astype(jnp.bfloat16)
    w_down_grad = jnp.dot(activation.T, grad_mlp, preferred_element_type=jnp.float32)
    grad_act = jnp.dot(grad_mlp, w_down.T, preferred_element_type=jnp.float32)
    grad_gate = (grad_act * up_proj * sigmoid_gate * (1.0 + gate_pre * (1.0 - sigmoid_gate))).astype(jnp.bfloat16)
    grad_up = (grad_act * gate_pre * sigmoid_gate).astype(jnp.bfloat16)
    w_gate_grad = jnp.dot(normed_two.T, grad_gate, preferred_element_type=jnp.float32)
    w_up_grad = jnp.dot(normed_two.T, grad_up, preferred_element_type=jnp.float32)
    grad_normed_two = jnp.dot(grad_gate, w_gate.T, preferred_element_type=jnp.float32) + jnp.dot(grad_up, w_up.T, preferred_element_type=jnp.float32)
    mlp_gain_grad = lax.optimization_barrier(jnp.sum(grad_normed_two * unit_two, axis=0))
    grad_hidden = grad_out + norm_backward(grad_normed_two, unit_two, scale_two, gain_two)
    grad_attn = (grad_hidden * valid_col).astype(jnp.bfloat16)
    w_output_grad = jnp.dot(attended_flat.T, grad_attn, preferred_element_type=jnp.float32)
    grad_attended = jnp.dot(grad_attn, w_output.T, preferred_element_type=jnp.float32).astype(jnp.bfloat16)
    grad_attended = grad_attended.reshape(total_rows, kv_heads, group_size, HEAD_SIZE)
    query_grad, key_grad, value_grad = attention_backward(queries, keys_rot, values, attended, grad_attended, log_total, document_segment, QBLK)
    query_back = rotate(query_grad, cosine, sine_part, -1.0).astype(jnp.bfloat16).reshape(total_rows, head_count * HEAD_SIZE)
    key_back = rotate(key_grad, cosine, sine_part, -1.0).astype(jnp.bfloat16).reshape(total_rows, kv_heads * HEAD_SIZE)
    value_back = value_grad.astype(jnp.bfloat16).reshape(total_rows, kv_heads * HEAD_SIZE)
    grad_normed_one = jnp.dot(query_back, w_query.T, preferred_element_type=jnp.float32) + jnp.dot(key_back, w_key.T, preferred_element_type=jnp.float32) + jnp.dot(value_back, value_weight.T, preferred_element_type=jnp.float32)
    w_query_grad = jnp.dot(normed_one.T, query_back, preferred_element_type=jnp.float32)
    w_key_grad = jnp.dot(normed_one.T, key_back, preferred_element_type=jnp.float32)
    w_value_grad = jnp.dot(normed_one.T, value_back, preferred_element_type=jnp.float32)
    attn_gain_grad = lax.optimization_barrier(jnp.sum(grad_normed_one * unit_one, axis=0))
    input_grad = grad_hidden + norm_backward(grad_normed_one, unit_one, scale_one, gain_one)
    grads = (attn_gain_grad, w_query_grad, w_key_grad, w_value_grad, w_output_grad, mlp_gain_grad, w_gate_grad, w_up_grad, w_down_grad)
    return (output, input_grad, grads)

def reference(inputs, doc_lengths, attn_gain, w_query, w_key, value_weight, w_output, mlp_gain, w_gate, w_up, w_down, out_grad):
    params = (attn_gain, w_query, w_key, value_weight, w_output, mlp_gain, w_gate, w_up, w_down)
    zero_grads = tuple((jnp.zeros(weight_item.shape, jnp.float32) for weight_item in params))
    grouped_inputs = inputs.reshape(N_DP, ROWS, MODEL_WIDTH)
    grouped_grad = out_grad.reshape(N_DP, ROWS, MODEL_WIDTH)

    def one_group(totals, pieces):
        group_inputs, group_lengths, group_grad = pieces
        output, input_grad, grads = layer_group(group_inputs, group_lengths, group_grad, params)
        return (jax.tree.map(jnp.add, totals, grads), (output, input_grad))
    totals, (outputs, input_grads) = lax.scan(one_group, zero_grads, (grouped_inputs, doc_lengths, grouped_grad))
    return (outputs.reshape(TOKENS, MODEL_WIDTH), input_grads.reshape(TOKENS, MODEL_WIDTH), totals[0], totals[1], totals[2], totals[3], totals[4], totals[5], totals[6], totals[7], totals[8])
```

```python
import jax
import jax.numpy as jnp
from jax import lax
from jax.sharding import PartitionSpec as P


HEAD_SIZE = 64
QBLK = 512


epsilon = 1e-05
rope_base = 500000.0


def layout(lengths, total_rows):
    row_index = jnp.arange(total_rows, dtype=jnp.int32)
    doc_ends = jnp.cumsum(lengths)
    passed = doc_ends[None, :] <= row_index[:, None]
    document_segment = jnp.sum(passed.astype(jnp.int32), axis=1)
    doc_start = jnp.sum(jnp.where(passed, lengths[None, :], 0), axis=1)
    positions = (row_index - doc_start).astype(jnp.float32)
    valid_rows = (document_segment < lengths.shape[0]).astype(jnp.float32)
    return (document_segment, positions, valid_rows)


def rope_tables(positions, head_dim):
    half_dim = head_dim // 2
    inverse_freq = rope_base ** (-(jnp.arange(half_dim, dtype=jnp.float32) * 2.0 / head_dim))
    angles = positions[:, None] * inverse_freq[None, :]
    return (jnp.cos(angles)[:, None, :], jnp.sin(angles)[:, None, :])


def rotate(tensor, cosine, sine_part, direction):
    half_dim = tensor.shape[-1] // 2
    first_half = tensor[..., :half_dim]
    second_half = tensor[..., half_dim:]
    return jnp.concatenate(
        [
            first_half * cosine - direction * second_half * sine_part,
            second_half * cosine + direction * first_half * sine_part,
        ],
        axis=-1,
    )


def rms_stats(hidden):
    scale_row = lax.rsqrt(jnp.mean(hidden * hidden, axis=-1, keepdims=True) + epsilon)
    return (scale_row, hidden * scale_row)


def norm_backward(grad_normed, unit_rows, scale_row, gain_wide):
    scaled = grad_normed * gain_wide
    return scale_row * (scaled - unit_rows * jnp.mean(scaled * unit_rows, axis=-1, keepdims=True))


def block_mask(document_segment, first_row, block_rows):
    row_index = jnp.arange(document_segment.shape[0], dtype=jnp.int32)
    query_rows = first_row + jnp.arange(block_rows, dtype=jnp.int32)
    query_segment = lax.dynamic_slice_in_dim(document_segment, first_row, block_rows, 0)
    return (query_segment[:, None] == document_segment[None, :]) & (
        row_index[None, :] <= query_rows[:, None]
    )


def attention_forward(queries, keys_rot, values, document_segment, block_rows):
    total_rows, kv_heads, group_size, head_dim = queries.shape
    score_scale = head_dim ** (-0.5)

    def one_block(block_index):
        first_row = block_index * block_rows
        query_block = lax.dynamic_slice_in_dim(queries, first_row, block_rows, 0)
        allowed = block_mask(document_segment, first_row, block_rows)
        scores = (
            jnp.einsum("qkgd,skd->kgqs", query_block, keys_rot, preferred_element_type=jnp.float32)
            * score_scale
        )
        scores = jnp.where(allowed, scores, -jnp.inf)
        row_max = jnp.max(scores, axis=-1, keepdims=True)
        log_total = row_max + jnp.log(jnp.sum(jnp.exp(scores - row_max), axis=-1, keepdims=True))
        weights = jnp.exp(scores - log_total).astype(jnp.bfloat16)
        attended = jnp.einsum("kgqs,skd->qkgd", weights, values, preferred_element_type=jnp.float32)
        return (attended.astype(jnp.bfloat16), log_total[..., 0])

    attended, log_total = lax.map(one_block, jnp.arange(total_rows // block_rows, dtype=jnp.int32))
    return (attended.reshape(total_rows, kv_heads, group_size, head_dim), log_total)


def attention_backward(
    queries, keys_rot, values, attended, grad_attended, log_total, document_segment, block_rows
):
    total_rows, kv_heads, group_size, head_dim = queries.shape
    score_scale = head_dim ** (-0.5)

    def one_block(running, block_index):
        key_grad, value_grad = running
        first_row = block_index * block_rows
        query_block = lax.dynamic_slice_in_dim(queries, first_row, block_rows, 0)
        block_gradient = lax.dynamic_slice_in_dim(grad_attended, first_row, block_rows, 0)
        out_block = lax.dynamic_slice_in_dim(attended, first_row, block_rows, 0)
        allowed = block_mask(document_segment, first_row, block_rows)
        scores = (
            jnp.einsum("qkgd,skd->kgqs", query_block, keys_rot, preferred_element_type=jnp.float32)
            * score_scale
        )
        scores = jnp.where(allowed, scores, -jnp.inf)
        prob_full = jnp.exp(scores - log_total[block_index][..., None])
        weights = prob_full.astype(jnp.bfloat16)
        value_grad = value_grad + jnp.einsum(
            "kgqs,qkgd->skd", weights, block_gradient, preferred_element_type=jnp.float32
        )
        grad_probs = jnp.einsum(
            "qkgd,skd->kgqs", block_gradient, values, preferred_element_type=jnp.float32
        )
        row_delta = jnp.einsum(
            "qkgd,qkgd->kgq", block_gradient, out_block, preferred_element_type=jnp.float32
        )
        grad_scores = (prob_full * (grad_probs - row_delta[..., None])).astype(jnp.bfloat16)
        query_grad = (
            jnp.einsum("kgqs,skd->qkgd", grad_scores, keys_rot, preferred_element_type=jnp.float32)
            * score_scale
        )
        key_grad = (
            key_grad
            + jnp.einsum(
                "kgqs,qkgd->skd", grad_scores, query_block, preferred_element_type=jnp.float32
            )
            * score_scale
        )
        return ((key_grad, value_grad), query_grad)

    zero_keys = jnp.zeros((total_rows, kv_heads, head_dim), jnp.float32)
    (key_grad, value_grad), query_grad = lax.scan(
        one_block, (zero_keys, zero_keys), jnp.arange(total_rows // block_rows, dtype=jnp.int32)
    )
    return (query_grad.reshape(total_rows, kv_heads * group_size, head_dim), key_grad, value_grad)


def shift_pairs(count, mask):
    return [(i, i ^ mask) for i in range(count)]


def gather_rows_plain(block, axis):
    count = lax.axis_size(axis)
    if count != 4:
        return lax.all_gather(block, axis, axis=0, tiled=True)
    me = lax.axis_index(axis)
    rows = block.shape[0]
    half = rows // 2
    from_x = lax.ppermute(block, axis, shift_pairs(count, 1))
    from_y = lax.ppermute(block, axis, shift_pairs(count, 2))
    far_top = lax.ppermute(from_x[:half], axis, shift_pairs(count, 2))
    far_low = lax.ppermute(from_y[half:], axis, shift_pairs(count, 1))
    whole = jnp.zeros((count * rows, block.shape[1]), block.dtype)
    for mask, piece, extra in (
        (0, block, 0),
        (1, from_x, 0),
        (2, from_y, 0),
        (3, far_top, 0),
        (3, far_low, half),
    ):
        whole = lax.dynamic_update_slice(whole, piece, ((me ^ mask) * rows + extra, 0))
    return whole


def scatter_rows_plain(partial, axis):
    count = lax.axis_size(axis)
    if count != 4:
        return lax.psum_scatter(partial, axis, scatter_dimension=0, tiled=True).astype(jnp.float32)
    me = lax.axis_index(axis)
    rows = partial.shape[0] // count
    half = rows // 2

    def part(mask, extra):
        return lax.dynamic_slice_in_dim(partial, (me ^ mask) * rows + extra, half, 0)

    def send(piece, mask):
        return lax.ppermute(piece, axis, shift_pairs(count, mask))

    relay_top = send(part(3, 0), 1).astype(jnp.float32)
    relay_low = send(part(3, half), 2).astype(jnp.float32)
    near_top = send(part(1, 0), 1).astype(jnp.float32)
    near_low = send(part(2, half), 2).astype(jnp.float32)
    joined_top = send((part(2, 0) + relay_top).astype(jnp.bfloat16), 2).astype(jnp.float32)
    joined_low = send((part(1, half) + relay_low).astype(jnp.bfloat16), 1).astype(jnp.float32)
    return jnp.concatenate(
        [part(0, 0) + near_top + joined_top, part(0, half) + near_low + joined_low], axis=0
    )


def product(left, right):
    return jnp.dot(left, right, preferred_element_type=jnp.float32)


def ordered(*values):
    return lax.optimization_barrier(values)


def sum_shards(partial, dimension):
    return lax.psum_scatter(partial, "dp", scatter_dimension=dimension, tiled=True)


def narrow(value):
    return value.astype(jnp.bfloat16)


def whole_block(
    inputs,
    doc_lengths,
    attn_gain,
    w_query,
    w_key,
    value_weight,
    w_output,
    mlp_gain,
    w_gate,
    w_up,
    w_down,
    out_grad,
):
    tensor_rank = lax.axis_index("tensor")
    own_rows = inputs.shape[0]
    total_rows = own_rows * lax.axis_size("tensor")
    query_cols, key_cols = w_query.shape[1], w_key.shape[1]
    joint = query_cols + 2 * key_cols
    document_segment, positions, valid_rows = layout(doc_lengths[0], total_rows)
    valid_own = lax.dynamic_slice_in_dim(valid_rows, tensor_rank * own_rows, own_rows, 0)[:, None]
    cosine, sine_part = rope_tables(positions, HEAD_SIZE)
    gains = jnp.pad(jnp.stack([attn_gain, mlp_gain], axis=1), ((0, 0), (0, 126)))
    packed = lax.all_gather(
        jnp.concatenate([w_query, w_key, value_weight, gains], axis=1), "dp", axis=0, tiled=True
    )
    full_joint = packed[:, :joint]
    gain_one = packed[:, joint].astype(jnp.float32)
    gain_two = packed[:, joint + 1].astype(jnp.float32)
    full_output = lax.all_gather(w_output, "dp", axis=1, tiled=True)
    full_gate = lax.all_gather(w_gate, "dp", axis=0, tiled=True)
    full_up = lax.all_gather(w_up, "dp", axis=0, tiled=True)
    full_down = lax.all_gather(w_down, "dp", axis=1, tiled=True)

    grad_out = out_grad.astype(jnp.float32)
    head_count = query_cols // HEAD_SIZE
    kv_heads = key_cols // HEAD_SIZE
    group_size = head_count // kv_heads
    residual = inputs.astype(jnp.float32)
    scale_one, unit_one = rms_stats(residual)
    inputs_all = gather_rows_plain(inputs, "tensor")
    cotangent_all = gather_rows_plain(out_grad, "tensor")
    normed_one_all = narrow(rms_stats(inputs_all.astype(jnp.float32))[1] * gain_one)
    grad_mlp_all = cotangent_all * narrow(valid_rows)[:, None]
    joint_full = product(normed_one_all, full_joint)
    query_full = joint_full[:, :query_cols].reshape(total_rows, head_count, HEAD_SIZE)
    key_full = joint_full[:, query_cols : query_cols + key_cols].reshape(
        total_rows, kv_heads, HEAD_SIZE
    )
    queries = narrow(rotate(query_full, cosine, sine_part, 1.0)).reshape(
        total_rows, kv_heads, group_size, HEAD_SIZE
    )
    keys_rot = narrow(rotate(key_full, cosine, sine_part, 1.0))
    values = narrow(joint_full[:, query_cols + key_cols :]).reshape(total_rows, kv_heads, HEAD_SIZE)
    attended, log_total = attention_forward(queries, keys_rot, values, document_segment, QBLK)
    attended_flat = attended.reshape(total_rows, query_cols)
    attn_out = scatter_rows_plain(narrow(product(attended_flat, full_output)), "tensor")
    hidden = residual + valid_own * attn_out
    scale_two, unit_two = rms_stats(hidden)
    normed_two_all = gather_rows_plain(narrow(unit_two * gain_two), "tensor")
    gate_pre = product(normed_two_all, full_gate)
    up_proj = product(normed_two_all, full_up)
    sigmoid_gate = jax.nn.sigmoid(gate_pre)
    activation = narrow(gate_pre * sigmoid_gate * up_proj)
    down_part = narrow(product(activation.T, grad_mlp_all))
    gate_pre, up_proj, down_part = ordered(gate_pre, up_proj, down_part)
    w_down_grad = sum_shards(down_part, 1)
    sigmoid_gate = jax.nn.sigmoid(gate_pre)
    grad_act = product(grad_mlp_all, full_down.T)
    grad_gate = narrow(grad_act * up_proj * sigmoid_gate * (1.0 + gate_pre * (1.0 - sigmoid_gate)))
    grad_up = narrow(grad_act * gate_pre * sigmoid_gate)
    normed_part = narrow(product(grad_gate, full_gate.T) + product(grad_up, full_up.T))
    grad_gate, grad_up, normed_part = ordered(grad_gate, grad_up, normed_part)
    grad_normed_two = scatter_rows_plain(normed_part, "tensor")
    gate_part = narrow(product(normed_two_all.T, grad_gate))
    up_part = narrow(product(normed_two_all.T, grad_up))
    grad_normed_two, gate_part, up_part = ordered(grad_normed_two, gate_part, up_part)
    w_gate_grad = sum_shards(gate_part, 0)
    w_up_grad = sum_shards(up_part, 0)
    mlp_gain_part = jnp.sum(grad_normed_two * unit_two, axis=0)
    grad_hidden = grad_out + norm_backward(grad_normed_two, unit_two, scale_two, gain_two)
    grad_attn = narrow(grad_hidden * valid_own)
    activation, grad_attn = ordered(activation, grad_attn)
    grad_attn_all = gather_rows_plain(grad_attn, "tensor")
    mlp_part = narrow(product(activation, full_down))
    grad_attn_all, mlp_part = ordered(grad_attn_all, mlp_part)
    mlp_out = scatter_rows_plain(mlp_part, "tensor")
    output = hidden + valid_own * mlp_out
    w_output_grad = sum_shards(narrow(product(attended_flat.T, grad_attn_all)), 1)
    grad_attended = narrow(product(grad_attn_all, full_output.T)).reshape(
        total_rows, kv_heads, group_size, HEAD_SIZE
    )
    query_grad, key_grad, value_grad = attention_backward(
        queries, keys_rot, values, attended, grad_attended, log_total, document_segment, QBLK
    )
    joint_back = jnp.concatenate(
        [
            narrow(rotate(query_grad, cosine, sine_part, -1.0)).reshape(total_rows, query_cols),
            narrow(rotate(key_grad, cosine, sine_part, -1.0)).reshape(total_rows, key_cols),
            narrow(value_grad).reshape(total_rows, key_cols),
        ],
        axis=1,
    )
    joint_grad = sum_shards(narrow(product(normed_one_all.T, joint_back)), 0).astype(jnp.float32)
    grad_normed_one = scatter_rows_plain(narrow(product(joint_back, full_joint.T)), "tensor")
    attn_gain_part = jnp.sum(grad_normed_one * unit_one, axis=0)
    input_grad = grad_hidden + norm_backward(grad_normed_one, unit_one, scale_one, gain_one)
    gain_sums = lax.psum(jnp.stack([attn_gain_part, mlp_gain_part]), ("dp", "tensor"))
    gain_rows = attn_gain.shape[0]
    gain_own = lax.dynamic_slice_in_dim(gain_sums, lax.axis_index("dp") * gain_rows, gain_rows, 1)
    return (
        output,
        input_grad,
        gain_own[0],
        joint_grad[:, :query_cols],
        joint_grad[:, query_cols : query_cols + key_cols],
        joint_grad[:, query_cols + key_cols :],
        w_output_grad.astype(jnp.float32),
        gain_own[1],
        w_gate_grad.astype(jnp.float32),
        w_up_grad.astype(jnp.float32),
        w_down_grad.astype(jnp.float32),
    )


def solution(mesh):
    placed = (
        P(("dp", "tensor"), None),
        P("dp", None),
        P("dp"),
        P("dp", "tensor"),
        P("dp", "tensor"),
        P("dp", "tensor"),
        P("tensor", "dp"),
        P("dp"),
        P("dp", "tensor"),
        P("dp", "tensor"),
        P("tensor", "dp"),
        P(("dp", "tensor"), None),
    )
    return jax.shard_map(
        whole_block,
        mesh=mesh,
        in_specs=placed,
        out_specs=(
            P(("dp", "tensor"), None),
            P(("dp", "tensor"), None),
            P("dp"),
            P("dp", "tensor"),
            P("dp", "tensor"),
            P("dp", "tensor"),
            P("tensor", "dp"),
            P("dp"),
            P("dp", "tensor"),
            P("dp", "tensor"),
            P("tensor", "dp"),
        ),
        check_vma=False,
    )
```

```python
import functools

import jax
import jax.numpy as jnp
from jax import lax
from jax.experimental import pallas as pl
from jax.experimental.pallas import tpu as pltpu
from jax.sharding import PartitionSpec as P


HEAD_SIZE = 64
QBLK = 256


epsilon = 1e-05
rope_base = 500000.0


def layout(lengths, total_rows):
    row_index = jnp.arange(total_rows, dtype=jnp.int32)
    doc_ends = jnp.cumsum(lengths)
    passed = doc_ends[None, :] <= row_index[:, None]
    document_segment = jnp.sum(passed.astype(jnp.int32), axis=1)
    doc_start = jnp.sum(jnp.where(passed, lengths[None, :], 0), axis=1)
    positions = (row_index - doc_start).astype(jnp.float32)
    valid_rows = (document_segment < lengths.shape[0]).astype(jnp.float32)
    return (document_segment, positions, valid_rows)


def rope_tables(positions, head_dim):
    half_dim = head_dim // 2
    inverse_freq = rope_base ** (-(jnp.arange(half_dim, dtype=jnp.float32) * 2.0 / head_dim))
    angles = positions[None, :] * inverse_freq[:, None]
    return (jnp.cos(angles), jnp.sin(angles))


def rms_stats(hidden):
    scale_row = lax.rsqrt(jnp.mean(hidden * hidden, axis=-1, keepdims=True) + epsilon)
    return (scale_row, hidden * scale_row)


def norm_backward(grad_normed, unit_rows, scale_row, gain_wide):
    scaled = grad_normed * gain_wide
    return scale_row * (scaled - unit_rows * jnp.mean(scaled * unit_rows, axis=-1, keepdims=True))


def rope_rows(ref, base, cosine, sine_part):
    half = HEAD_SIZE // 2
    first = ref[pl.ds(base, half), :]
    second = ref[pl.ds(base + half, half), :]
    return first * cosine - second * sine_part, second * cosine + first * sine_part


def fill_bias(bias_ref, seg_row_ref, seg_col_ref, start, block):
    keys = start + block
    key_index = lax.broadcasted_iota(jnp.int32, (keys, block), 0)
    query_index = lax.broadcasted_iota(jnp.int32, (keys, block), 1) + start
    allowed = (seg_col_ref[:keys, :] == seg_row_ref[:, start : start + block]) & (
        key_index <= query_index
    )
    bias_ref[:keys, :] = jnp.where(allowed, 0.0, -jnp.inf)


def head_base(index):
    return pl.multiple_of(index * HEAD_SIZE, HEAD_SIZE)


def turned(value):
    return jnp.transpose(value.astype(jnp.float32)).astype(jnp.bfloat16)


def attend_kernel(
    heads, kv_heads, block, joint_ref, cos_ref, sin_ref, seg_row_ref, seg_col_ref,
    rot_ref, att_ref, log_ref, krow_ref, bias_ref,
):
    rows = joint_ref.shape[1]
    half = HEAD_SIZE // 2
    group = heads // kv_heads
    value_base = (heads + kv_heads) * HEAD_SIZE

    def rotate_head(index, scale):
        base = head_base(index)
        first, second = rope_rows(joint_ref, base, cos_ref[...], sin_ref[...])
        rot_ref[pl.ds(base, half), :] = (first * scale).astype(jnp.bfloat16)
        rot_ref[pl.ds(base + half, half), :] = (second * scale).astype(jnp.bfloat16)

    @pl.loop(0, heads)
    def _(index):
        rotate_head(index, HEAD_SIZE ** (-0.5))

    @pl.loop(0, kv_heads)
    def _(index):
        rotate_head(heads + index, 1.0)
        krow_ref[index] = turned(rot_ref[pl.ds(head_base(heads + index), HEAD_SIZE), :])

    rot_ref[value_base:, :] = joint_ref[value_base:, :].astype(jnp.bfloat16)
    for start in range(0, rows, block):
        keys = start + block
        fill_bias(bias_ref, seg_row_ref, seg_col_ref, start, block)

        @pl.loop(0, heads)
        def _(head):
            kv_head = head // group
            query = rot_ref[pl.ds(head_base(head), HEAD_SIZE), start:keys]
            scores = (
                jnp.dot(krow_ref[kv_head, :keys, :], query, preferred_element_type=jnp.float32)
                + bias_ref[:keys, :]
            )
            top = jnp.max(scores, axis=0, keepdims=True)
            powers = jnp.exp(scores - top)
            total = jnp.sum(powers, axis=0, keepdims=True)
            weights = (powers * (1.0 / total)).astype(jnp.bfloat16)
            value = rot_ref[pl.ds(head_base(heads + kv_heads + kv_head), HEAD_SIZE), :keys]
            att_ref[pl.ds(head_base(head), HEAD_SIZE), start:keys] = jnp.dot(
                value, weights, preferred_element_type=jnp.float32
            ).astype(jnp.bfloat16)
            log_ref[pl.ds(head, 1), start:keys] = top + jnp.log(total)


def attend_back_kernel(
    heads, kv_heads, block, rot_ref, att_ref, out_ref, log_ref, cos_ref, sin_ref,
    seg_row_ref, seg_col_ref, back_ref, krow_ref, vrow_ref, dkey_ref, dvalue_ref, bias_ref,
):
    rows = rot_ref.shape[1]
    half = HEAD_SIZE // 2
    group = heads // kv_heads
    last = (((1,), (1,)), ((), ()))

    def turn_back(first, second, base, start, stop):
        cosine, sine_part = cos_ref[:, start:stop], sin_ref[:, start:stop]
        back_ref[pl.ds(base, half), start:stop] = (
            first * cosine + second * sine_part
        ).astype(jnp.bfloat16)
        back_ref[pl.ds(base + half, half), start:stop] = (
            second * cosine - first * sine_part
        ).astype(jnp.bfloat16)

    @pl.loop(0, kv_heads)
    def _(index):
        krow_ref[index] = turned(rot_ref[pl.ds(head_base(heads + index), HEAD_SIZE), :])
        vrow_ref[index] = turned(rot_ref[pl.ds(head_base(heads + kv_heads + index), HEAD_SIZE), :])

    dkey_ref[...] = jnp.zeros_like(dkey_ref)
    dvalue_ref[...] = jnp.zeros_like(dvalue_ref)
    for start in range(0, rows, block):
        keys = start + block
        fill_bias(bias_ref, seg_row_ref, seg_col_ref, start, block)

        @pl.loop(0, heads)
        def _(head):
            kv_head = head // group
            own = pl.ds(head_base(head), HEAD_SIZE)
            query = rot_ref[own, start:keys]
            grad = out_ref[own, start:keys]
            delta = jnp.sum(
                grad.astype(jnp.float32) * att_ref[own, start:keys].astype(jnp.float32),
                axis=0,
                keepdims=True,
            )
            scores = (
                jnp.dot(krow_ref[kv_head, :keys, :], query, preferred_element_type=jnp.float32)
                + bias_ref[:keys, :]
            )
            probs = jnp.exp(scores - log_ref[pl.ds(head, 1), start:keys])
            grad_probs = jnp.dot(
                vrow_ref[kv_head, :keys, :], grad, preferred_element_type=jnp.float32
            )
            grad_scores = (probs * (grad_probs - delta)).astype(jnp.bfloat16)
            dvalue_ref[kv_head, :keys, :] += lax.dot_general(
                probs.astype(jnp.bfloat16), grad, last, preferred_element_type=jnp.float32
            )
            dkey_ref[kv_head, :keys, :] += lax.dot_general(
                grad_scores, query, last, preferred_element_type=jnp.float32
            )
            key = rot_ref[pl.ds(head_base(heads + kv_head), HEAD_SIZE), :keys]
            dquery = jnp.dot(key, grad_scores, preferred_element_type=jnp.float32) * (
                HEAD_SIZE ** (-0.5)
            )
            turn_back(dquery[:half], dquery[half:], head_base(head), start, keys)

    @pl.loop(0, kv_heads)
    def _(index):
        dkey = jnp.transpose(dkey_ref[index])
        turn_back(dkey[:half], dkey[half:], head_base(heads + index), 0, rows)
        back_ref[pl.ds(head_base(heads + kv_heads + index), HEAD_SIZE), :] = jnp.transpose(
            dvalue_ref[index]
        ).astype(jnp.bfloat16)


def activation_back_kernel(pair_ref, grad_ref, out_ref):
    units = grad_ref.shape[1]
    gate, up = pair_ref[:, :units], pair_ref[:, units:]
    grad = grad_ref[...]
    sigmoid_gate = 1.0 / (1.0 + jnp.exp(-gate))
    grad_gate = grad * up * sigmoid_gate * (1.0 + gate * (1.0 - sigmoid_gate))
    out_ref[:, :units] = grad_gate.astype(jnp.bfloat16)
    out_ref[:, units:] = (grad * gate * sigmoid_gate).astype(jnp.bfloat16)


def activation_back(pair, grad):
    rows, units = grad.shape
    block = min(rows, 128)

    def at(row):
        return (row, 0)

    return pl.pallas_call(
        activation_back_kernel,
        out_shape=jax.ShapeDtypeStruct(pair.shape, jnp.bfloat16),
        grid=(rows // block,),
        in_specs=[pl.BlockSpec((block, 2 * units), at), pl.BlockSpec((block, units), at)],
        out_specs=pl.BlockSpec((block, 2 * units), at),
        cost_estimate=pl.CostEstimate(
            flops=20 * pair.size, bytes_accessed=8 * pair.size, transcendentals=pair.size
        ),
        name="activation_back",
    )(pair, grad)


def in_vmem(count):
    return [pl.BlockSpec(memory_space=pltpu.VMEM)] * count


def attend(joint, cosine, sine_part, seg_row, seg_col, heads, kv_heads, block):
    rows = joint.shape[1]
    flops = 2 * heads * rows * rows * HEAD_SIZE
    return pl.pallas_call(
        functools.partial(attend_kernel, heads, kv_heads, block),
        out_shape=(
            jax.ShapeDtypeStruct(joint.shape, jnp.bfloat16),
            jax.ShapeDtypeStruct((heads * HEAD_SIZE, rows), jnp.bfloat16),
            jax.ShapeDtypeStruct((heads, rows), jnp.float32),
        ),
        in_specs=in_vmem(5),
        out_specs=tuple(in_vmem(3)),
        scratch_shapes=[
            pltpu.VMEM((kv_heads, rows, HEAD_SIZE), jnp.bfloat16),
            pltpu.VMEM((rows, block), jnp.float32),
        ],
        cost_estimate=pl.CostEstimate(
            flops=8 * flops, bytes_accessed=8 * joint.size, transcendentals=heads * rows * rows
        ),
        name="attend",
    )(joint, cosine, sine_part, seg_row, seg_col)


def attend_back(rotated, attended, grad, log_total, cosine, sine_part, seg_row, seg_col, heads, kv_heads, block):
    rows = rotated.shape[1]
    flops = 2 * heads * rows * rows * HEAD_SIZE
    return pl.pallas_call(
        functools.partial(attend_back_kernel, heads, kv_heads, block),
        out_shape=jax.ShapeDtypeStruct(rotated.shape, jnp.bfloat16),
        in_specs=in_vmem(8),
        out_specs=pl.BlockSpec(memory_space=pltpu.VMEM),
        scratch_shapes=[
            pltpu.VMEM((kv_heads, rows, HEAD_SIZE), jnp.bfloat16),
            pltpu.VMEM((kv_heads, rows, HEAD_SIZE), jnp.bfloat16),
            pltpu.VMEM((kv_heads, rows, HEAD_SIZE), jnp.float32),
            pltpu.VMEM((kv_heads, rows, HEAD_SIZE), jnp.float32),
            pltpu.VMEM((rows, block), jnp.float32),
        ],
        cost_estimate=pl.CostEstimate(
            flops=20 * flops, bytes_accessed=8 * rotated.size, transcendentals=heads * rows * rows
        ),
        name="attend_back",
    )(rotated, attended, grad, log_total, cosine, sine_part, seg_row, seg_col)


def shift_pairs(count, mask):
    return [(i, i ^ mask) for i in range(count)]


def gather_rows_plain(block, axis):
    count = lax.axis_size(axis)
    if count != 4:
        return lax.all_gather(block, axis, axis=0, tiled=True)
    me = lax.axis_index(axis)
    rows = block.shape[0]
    half = rows // 2
    from_x = lax.ppermute(block, axis, shift_pairs(count, 1))
    from_y = lax.ppermute(block, axis, shift_pairs(count, 2))
    far_top = lax.ppermute(from_x[:half], axis, shift_pairs(count, 2))
    far_low = lax.ppermute(from_y[half:], axis, shift_pairs(count, 1))
    whole = jnp.zeros((count * rows, block.shape[1]), block.dtype)
    for mask, piece, extra in (
        (0, block, 0),
        (1, from_x, 0),
        (2, from_y, 0),
        (3, far_top, 0),
        (3, far_low, half),
    ):
        whole = lax.dynamic_update_slice(whole, piece, ((me ^ mask) * rows + extra, 0))
    return whole


def scatter_rows_plain(partial, axis):
    count = lax.axis_size(axis)
    if count != 4:
        return lax.psum_scatter(partial, axis, scatter_dimension=0, tiled=True).astype(jnp.float32)
    me = lax.axis_index(axis)
    rows = partial.shape[0] // count
    half = rows // 2

    def part(mask, extra):
        return lax.dynamic_slice_in_dim(partial, (me ^ mask) * rows + extra, half, 0)

    def send(piece, mask):
        return lax.ppermute(piece, axis, shift_pairs(count, mask))

    relay_top = send(part(3, 0), 1).astype(jnp.float32)
    relay_low = send(part(3, half), 2).astype(jnp.float32)
    near_top = send(part(1, 0), 1).astype(jnp.float32)
    near_low = send(part(2, half), 2).astype(jnp.float32)
    joined_top = send((part(2, 0) + relay_top).astype(jnp.bfloat16), 2).astype(jnp.float32)
    joined_low = send((part(1, half) + relay_low).astype(jnp.bfloat16), 1).astype(jnp.float32)
    return jnp.concatenate(
        [part(0, 0) + near_top + joined_top, part(0, half) + near_low + joined_low], axis=0
    )


def product(left, right):
    return jnp.dot(left, right, preferred_element_type=jnp.float32)


def contract(left, right, left_axis, right_axis):
    return lax.dot_general(
        left,
        right,
        (((left_axis,), (right_axis,)), ((), ())),
        preferred_element_type=jnp.float32,
    )


def ordered(*values):
    return lax.optimization_barrier(values)


def sum_shards(partial, dimension):
    return lax.psum_scatter(partial, "dp", scatter_dimension=dimension, tiled=True)


def narrow(value):
    return value.astype(jnp.bfloat16)


def whole_block(
    inputs,
    doc_lengths,
    attn_gain,
    w_query,
    w_key,
    value_weight,
    w_output,
    mlp_gain,
    w_gate,
    w_up,
    w_down,
    out_grad,
):
    tensor_rank = lax.axis_index("tensor")
    own_rows = inputs.shape[0]
    total_rows = own_rows * lax.axis_size("tensor")
    query_cols, key_cols = w_query.shape[1], w_key.shape[1]
    joint = query_cols + 2 * key_cols
    document_segment, positions, valid_rows = layout(doc_lengths[0], total_rows)
    valid_own = lax.dynamic_slice_in_dim(valid_rows, tensor_rank * own_rows, own_rows, 0)[:, None]
    cosine, sine_part = rope_tables(positions, HEAD_SIZE)
    gains = jnp.pad(jnp.stack([attn_gain, mlp_gain], axis=1), ((0, 0), (0, 126)))
    packed = lax.all_gather(
        jnp.concatenate([w_query, w_key, value_weight, gains, w_output.T], axis=1),
        "dp",
        axis=0,
        tiled=True,
    )
    full_joint = packed[:, :joint]
    gain_one = packed[:, joint].astype(jnp.float32)
    gain_two = packed[:, joint + 1].astype(jnp.float32)
    full_output = packed[:, joint + gains.shape[1] :]
    full_pair = lax.all_gather(
        jnp.concatenate([w_gate, w_up], axis=1), "dp", axis=0, tiled=True
    )
    full_down = lax.all_gather(w_down, "dp", axis=1, tiled=True)

    grad_out = out_grad.astype(jnp.float32)
    head_count = query_cols // HEAD_SIZE
    kv_heads = key_cols // HEAD_SIZE
    residual = inputs.astype(jnp.float32)
    scale_one, unit_one = rms_stats(residual)
    inputs_all = gather_rows_plain(inputs, "tensor")
    cotangent_all = gather_rows_plain(out_grad, "tensor")
    normed_one_all = narrow(rms_stats(inputs_all.astype(jnp.float32))[1] * gain_one)
    grad_mlp_all = cotangent_all * narrow(valid_rows)[:, None]
    seg_row, seg_col = document_segment[None, :], document_segment[:, None]
    joint_turned = contract(full_joint, normed_one_all, 0, 1)
    rotated, attended, log_total = attend(
        joint_turned, cosine, sine_part, seg_row, seg_col, head_count, kv_heads, QBLK
    )
    attn_out = scatter_rows_plain(narrow(contract(attended, full_output, 0, 1)), "tensor")
    hidden = residual + valid_own * attn_out
    scale_two, unit_two = rms_stats(hidden)
    normed_two_all = gather_rows_plain(narrow(unit_two * gain_two), "tensor")
    hidden_units = w_gate.shape[1]
    pair_pre = product(normed_two_all, full_pair)
    gate_pre, up_proj = pair_pre[:, :hidden_units], pair_pre[:, hidden_units:]
    activation = narrow(gate_pre * jax.nn.sigmoid(gate_pre) * up_proj)
    down_part = narrow(product(activation.T, grad_mlp_all))
    pair_pre, down_part = ordered(pair_pre, down_part)
    w_down_grad = sum_shards(down_part, 1)
    grad_act = product(grad_mlp_all, full_down.T)
    grad_pair = activation_back(pair_pre, grad_act)
    normed_part = narrow(contract(grad_pair, full_pair, 1, 1))
    grad_pair, normed_part = ordered(grad_pair, normed_part)
    grad_normed_two = scatter_rows_plain(normed_part, "tensor")
    pair_part = narrow(contract(normed_two_all, grad_pair, 0, 0))
    grad_normed_two, pair_part = ordered(grad_normed_two, pair_part)
    pair_grad = sum_shards(pair_part, 0).astype(jnp.float32)
    mlp_gain_part = jnp.sum(grad_normed_two * unit_two, axis=0)
    grad_hidden = grad_out + norm_backward(grad_normed_two, unit_two, scale_two, gain_two)
    grad_attn = narrow(grad_hidden * valid_own)
    activation, grad_attn = ordered(activation, grad_attn)
    grad_attn_all = gather_rows_plain(grad_attn, "tensor")
    mlp_part = narrow(product(activation, full_down))
    grad_attn_all, mlp_part = ordered(grad_attn_all, mlp_part)
    mlp_out = scatter_rows_plain(mlp_part, "tensor")
    output = hidden + valid_own * mlp_out
    out_part = narrow(contract(grad_attn_all, attended, 0, 1))
    grad_attended = narrow(contract(full_output, grad_attn_all, 0, 1))
    joint_back = attend_back(
        rotated,
        attended,
        grad_attended,
        log_total,
        cosine,
        sine_part,
        seg_row,
        seg_col,
        head_count,
        kv_heads,
        QBLK,
    )
    joint_part = narrow(contract(normed_one_all, joint_back, 0, 1))
    tail_grad = sum_shards(jnp.concatenate([joint_part, out_part], axis=1), 0).astype(jnp.float32)
    grad_normed_one = scatter_rows_plain(narrow(contract(joint_back, full_joint, 0, 1)), "tensor")
    attn_gain_part = jnp.sum(grad_normed_one * unit_one, axis=0)
    input_grad = grad_hidden + norm_backward(grad_normed_one, unit_one, scale_one, gain_one)
    gain_sums = lax.psum(jnp.stack([attn_gain_part, mlp_gain_part]), ("dp", "tensor"))
    gain_rows = attn_gain.shape[0]
    gain_own = lax.dynamic_slice_in_dim(gain_sums, lax.axis_index("dp") * gain_rows, gain_rows, 1)
    return (
        output,
        input_grad,
        gain_own[0],
        tail_grad[:, :query_cols],
        tail_grad[:, query_cols : query_cols + key_cols],
        tail_grad[:, query_cols + key_cols : joint],
        tail_grad[:, joint:].T,
        gain_own[1],
        pair_grad[:, :hidden_units],
        pair_grad[:, hidden_units:],
        w_down_grad.astype(jnp.float32),
    )


def solution(mesh):
    placed = (
        P(("dp", "tensor"), None),
        P("dp", None),
        P("dp"),
        P("dp", "tensor"),
        P("dp", "tensor"),
        P("dp", "tensor"),
        P("tensor", "dp"),
        P("dp"),
        P("dp", "tensor"),
        P("dp", "tensor"),
        P("tensor", "dp"),
        P(("dp", "tensor"), None),
    )
    return jax.shard_map(
        whole_block,
        mesh=mesh,
        in_specs=placed,
        out_specs=(
            P(("dp", "tensor"), None),
            P(("dp", "tensor"), None),
            P("dp"),
            P("dp", "tensor"),
            P("dp", "tensor"),
            P("dp", "tensor"),
            P("tensor", "dp"),
            P("dp"),
            P("dp", "tensor"),
            P("dp", "tensor"),
            P("tensor", "dp"),
        ),
        check_vma=False,
    )
```

```python
import functools

import jax
import jax.numpy as jnp
from jax import lax
from jax.experimental import pallas as pl
from jax.experimental.layout import Layout, with_layout_constraint
from jax.experimental.pallas import tpu as pltpu
from jax.sharding import PartitionSpec as P


HEAD_SIZE = 64
QBLK = 256


epsilon = 1e-05
rope_base = 500000.0


def layout(lengths, total_rows):
    row_index = jnp.arange(total_rows, dtype=jnp.int32)
    doc_ends = jnp.cumsum(lengths)
    passed = doc_ends[None, :] <= row_index[:, None]
    document_segment = jnp.sum(passed.astype(jnp.int32), axis=1)
    doc_start = jnp.sum(jnp.where(passed, lengths[None, :], 0), axis=1)
    positions = (row_index - doc_start).astype(jnp.float32)
    valid_rows = (document_segment < lengths.shape[0]).astype(jnp.float32)
    return (document_segment, positions, valid_rows)


def rope_tables(positions, head_dim):
    half_dim = head_dim // 2
    inverse_freq = rope_base ** (-(jnp.arange(half_dim, dtype=jnp.float32) * 2.0 / head_dim))
    angles = positions[None, :] * inverse_freq[:, None]
    return (jnp.cos(angles), jnp.sin(angles))


def rms_stats(hidden):
    scale_row = lax.rsqrt(jnp.mean(hidden * hidden, axis=-1, keepdims=True) + epsilon)
    return (scale_row, hidden * scale_row)


def norm_backward(grad_normed, unit_rows, scale_row, gain_wide):
    scaled = grad_normed * gain_wide
    return scale_row * (scaled - unit_rows * jnp.mean(scaled * unit_rows, axis=-1, keepdims=True))


def rope_rows(ref, base, cosine, sine_part):
    half = HEAD_SIZE // 2
    first = ref[pl.ds(base, half), :]
    second = ref[pl.ds(base + half, half), :]
    return first * cosine - second * sine_part, second * cosine + first * sine_part


def fill_bias(bias_ref, seg_row_ref, seg_col_ref, start, block):
    keys = start + block
    key_index = lax.broadcasted_iota(jnp.int32, (keys, block), 0)
    query_index = lax.broadcasted_iota(jnp.int32, (keys, block), 1) + start
    allowed = (seg_col_ref[:keys, :] == seg_row_ref[:, start : start + block]) & (
        key_index <= query_index
    )
    bias_ref[:keys, :] = jnp.where(allowed, 0.0, -jnp.inf)


def head_base(index):
    return pl.multiple_of(index * HEAD_SIZE, HEAD_SIZE)


def turned(value):
    return jnp.transpose(value.astype(jnp.float32)).astype(jnp.bfloat16)


def attend_kernel(
    heads, kv_heads, block, joint_ref, cos_ref, sin_ref, seg_row_ref, seg_col_ref,
    rot_ref, att_ref, log_ref, krow_ref, bias_ref,
):
    rows = joint_ref.shape[1]
    half = HEAD_SIZE // 2
    group = heads // kv_heads
    value_base = (heads + kv_heads) * HEAD_SIZE

    def rotate_head(index, scale):
        base = head_base(index)
        first, second = rope_rows(joint_ref, base, cos_ref[...], sin_ref[...])
        rot_ref[pl.ds(base, half), :] = (first * scale).astype(jnp.bfloat16)
        rot_ref[pl.ds(base + half, half), :] = (second * scale).astype(jnp.bfloat16)

    @pl.loop(0, heads)
    def _(index):
        rotate_head(index, HEAD_SIZE ** (-0.5))

    @pl.loop(0, kv_heads)
    def _(index):
        rotate_head(heads + index, 1.0)
        krow_ref[index] = turned(rot_ref[pl.ds(head_base(heads + index), HEAD_SIZE), :])

    rot_ref[value_base:, :] = joint_ref[value_base:, :].astype(jnp.bfloat16)
    for start in range(0, rows, block):
        keys = start + block
        fill_bias(bias_ref, seg_row_ref, seg_col_ref, start, block)

        @pl.loop(0, heads)
        def _(head):
            kv_head = head // group
            query = rot_ref[pl.ds(head_base(head), HEAD_SIZE), start:keys]
            scores = (
                jnp.dot(krow_ref[kv_head, :keys, :], query, preferred_element_type=jnp.float32)
                + bias_ref[:keys, :]
            )
            top = jnp.max(scores, axis=0, keepdims=True)
            powers = jnp.exp(scores - top)
            total = jnp.sum(powers, axis=0, keepdims=True)
            weights = (powers * (1.0 / total)).astype(jnp.bfloat16)
            value = rot_ref[pl.ds(head_base(heads + kv_heads + kv_head), HEAD_SIZE), :keys]
            att_ref[pl.ds(head_base(head), HEAD_SIZE), start:keys] = jnp.dot(
                value, weights, preferred_element_type=jnp.float32
            ).astype(jnp.bfloat16)
            log_ref[pl.ds(head, 1), start:keys] = top + jnp.log(total)


def attend_back_kernel(
    heads, kv_heads, block, rot_ref, att_ref, out_ref, log_ref, cos_ref, sin_ref,
    seg_row_ref, seg_col_ref, back_ref, krow_ref, vrow_ref, dkey_ref, dvalue_ref, bias_ref,
):
    rows = rot_ref.shape[1]
    half = HEAD_SIZE // 2
    group = heads // kv_heads
    last = (((1,), (1,)), ((), ()))

    def turn_back(first, second, base, start, stop):
        cosine, sine_part = cos_ref[:, start:stop], sin_ref[:, start:stop]
        back_ref[pl.ds(base, half), start:stop] = (
            first * cosine + second * sine_part
        ).astype(jnp.bfloat16)
        back_ref[pl.ds(base + half, half), start:stop] = (
            second * cosine - first * sine_part
        ).astype(jnp.bfloat16)

    @pl.loop(0, kv_heads)
    def _(index):
        krow_ref[index] = turned(rot_ref[pl.ds(head_base(heads + index), HEAD_SIZE), :])
        vrow_ref[index] = turned(rot_ref[pl.ds(head_base(heads + kv_heads + index), HEAD_SIZE), :])

    dkey_ref[...] = jnp.zeros_like(dkey_ref)
    dvalue_ref[...] = jnp.zeros_like(dvalue_ref)
    for start in range(0, rows, block):
        keys = start + block
        fill_bias(bias_ref, seg_row_ref, seg_col_ref, start, block)

        @pl.loop(0, heads)
        def _(head):
            kv_head = head // group
            own = pl.ds(head_base(head), HEAD_SIZE)
            query = rot_ref[own, start:keys]
            grad = out_ref[own, start:keys]
            delta = jnp.sum(
                grad.astype(jnp.float32) * att_ref[own, start:keys].astype(jnp.float32),
                axis=0,
                keepdims=True,
            )
            scores = (
                jnp.dot(krow_ref[kv_head, :keys, :], query, preferred_element_type=jnp.float32)
                + bias_ref[:keys, :]
            )
            probs = jnp.exp(scores - log_ref[pl.ds(head, 1), start:keys])
            grad_probs = jnp.dot(
                vrow_ref[kv_head, :keys, :], grad, preferred_element_type=jnp.float32
            )
            grad_scores = (probs * (grad_probs - delta)).astype(jnp.bfloat16)
            dvalue_ref[kv_head, :keys, :] += lax.dot_general(
                probs.astype(jnp.bfloat16), grad, last, preferred_element_type=jnp.float32
            )
            dkey_ref[kv_head, :keys, :] += lax.dot_general(
                grad_scores, query, last, preferred_element_type=jnp.float32
            )
            key = rot_ref[pl.ds(head_base(heads + kv_head), HEAD_SIZE), :keys]
            dquery = jnp.dot(key, grad_scores, preferred_element_type=jnp.float32) * (
                HEAD_SIZE ** (-0.5)
            )
            turn_back(dquery[:half], dquery[half:], head_base(head), start, keys)

    @pl.loop(0, kv_heads)
    def _(index):
        dkey = jnp.transpose(dkey_ref[index])
        turn_back(dkey[:half], dkey[half:], head_base(heads + index), 0, rows)
        back_ref[pl.ds(head_base(heads + kv_heads + index), HEAD_SIZE), :] = jnp.transpose(
            dvalue_ref[index]
        ).astype(jnp.bfloat16)


def activation_kernel(pair_ref, grad_ref, act_ref, out_ref):
    units = grad_ref.shape[1]
    gate, up = pair_ref[:, :units], pair_ref[:, units:]
    grad = grad_ref[...]
    sigmoid_gate = 1.0 / (1.0 + jnp.exp(-gate))
    act_ref[...] = (gate * sigmoid_gate * up).astype(jnp.bfloat16)
    grad_gate = grad * up * sigmoid_gate * (1.0 + gate * (1.0 - sigmoid_gate))
    out_ref[:, :units] = grad_gate.astype(jnp.bfloat16)
    out_ref[:, units:] = (grad * gate * sigmoid_gate).astype(jnp.bfloat16)


def activation_both(pair, grad):
    rows, units = grad.shape
    block = min(rows, 256)

    def at(row):
        return (row, 0)

    return pl.pallas_call(
        activation_kernel,
        out_shape=(
            jax.ShapeDtypeStruct(grad.shape, jnp.bfloat16),
            jax.ShapeDtypeStruct(pair.shape, jnp.bfloat16),
        ),
        grid=(rows // block,),
        in_specs=[pl.BlockSpec((block, 2 * units), at), pl.BlockSpec((block, units), at)],
        out_specs=(pl.BlockSpec((block, units), at), pl.BlockSpec((block, 2 * units), at)),
        cost_estimate=pl.CostEstimate(
            flops=20 * pair.size, bytes_accessed=9 * pair.size, transcendentals=pair.size
        ),
        name="activation_both",
    )(pair, grad)


def in_vmem(count):
    return [pl.BlockSpec(memory_space=pltpu.VMEM)] * count


def attend(joint, cosine, sine_part, seg_row, seg_col, heads, kv_heads, block):
    rows = joint.shape[1]
    flops = 2 * heads * rows * rows * HEAD_SIZE
    return pl.pallas_call(
        functools.partial(attend_kernel, heads, kv_heads, block),
        out_shape=(
            jax.ShapeDtypeStruct(joint.shape, jnp.bfloat16),
            jax.ShapeDtypeStruct((heads * HEAD_SIZE, rows), jnp.bfloat16),
            jax.ShapeDtypeStruct((heads, rows), jnp.float32),
        ),
        in_specs=in_vmem(5),
        out_specs=tuple(in_vmem(3)),
        scratch_shapes=[
            pltpu.VMEM((kv_heads, rows, HEAD_SIZE), jnp.bfloat16),
            pltpu.VMEM((rows, block), jnp.float32),
        ],
        cost_estimate=pl.CostEstimate(
            flops=8 * flops, bytes_accessed=8 * joint.size, transcendentals=heads * rows * rows
        ),
        name="attend",
    )(joint, cosine, sine_part, seg_row, seg_col)


def attend_back(rotated, attended, grad, log_total, cosine, sine_part, seg_row, seg_col, heads, kv_heads, block):
    rows = rotated.shape[1]
    flops = 2 * heads * rows * rows * HEAD_SIZE
    return pl.pallas_call(
        functools.partial(attend_back_kernel, heads, kv_heads, block),
        out_shape=jax.ShapeDtypeStruct(rotated.shape, jnp.bfloat16),
        in_specs=in_vmem(8),
        out_specs=pl.BlockSpec(memory_space=pltpu.VMEM),
        scratch_shapes=[
            pltpu.VMEM((kv_heads, rows, HEAD_SIZE), jnp.bfloat16),
            pltpu.VMEM((kv_heads, rows, HEAD_SIZE), jnp.bfloat16),
            pltpu.VMEM((kv_heads, rows, HEAD_SIZE), jnp.float32),
            pltpu.VMEM((kv_heads, rows, HEAD_SIZE), jnp.float32),
            pltpu.VMEM((rows, block), jnp.float32),
        ],
        cost_estimate=pl.CostEstimate(
            flops=20 * flops, bytes_accessed=8 * rotated.size, transcendentals=heads * rows * rows
        ),
        name="attend_back",
    )(rotated, attended, grad, log_total, cosine, sine_part, seg_row, seg_col)


def shift_pairs(count, mask):
    return [(i, i ^ mask) for i in range(count)]


def gather_rows(block, axis, relative=False):
    count = lax.axis_size(axis)
    if count != 4:
        return lax.all_gather(block, axis, axis=0, tiled=True)
    me = lax.axis_index(axis)
    rows = block.shape[0]
    half = rows // 2
    from_x = lax.ppermute(block, axis, shift_pairs(count, 1))
    from_y = lax.ppermute(block, axis, shift_pairs(count, 2))
    far_top = lax.ppermute(from_x[:half], axis, shift_pairs(count, 2))
    far_low = lax.ppermute(from_y[half:], axis, shift_pairs(count, 1))
    if relative:
        return jnp.concatenate([block, from_x, from_y, far_top, far_low], axis=0)
    whole = jnp.zeros((count * rows, block.shape[1]), block.dtype)
    for mask, piece, extra in (
        (0, block, 0),
        (1, from_x, 0),
        (2, from_y, 0),
        (3, far_top, 0),
        (3, far_low, half),
    ):
        whole = lax.dynamic_update_slice(whole, piece, ((me ^ mask) * rows + extra, 0))
    return row_major(whole)


def scatter_rows(partial, axis, relative=False):
    count = lax.axis_size(axis)
    if count != 4:
        return lax.psum_scatter(partial, axis, scatter_dimension=0, tiled=True).astype(jnp.float32)
    me = 0 if relative else lax.axis_index(axis)
    rows = partial.shape[0] // count
    half = rows // 2

    def part(mask, extra):
        return lax.dynamic_slice_in_dim(partial, (me ^ mask) * rows + extra, half, 0)

    def send(piece, mask):
        return lax.ppermute(piece, axis, shift_pairs(count, mask))

    relay_top = send(part(3, 0), 1).astype(jnp.float32)
    relay_low = send(part(3, half), 2).astype(jnp.float32)
    near_top = send(part(1, 0), 1).astype(jnp.float32)
    near_low = send(part(2, half), 2).astype(jnp.float32)
    joined_top = send(narrow(part(2, 0) + relay_top), 2).astype(jnp.float32)
    joined_low = send(narrow(part(1, half) + relay_low), 1).astype(jnp.float32)
    return jnp.concatenate(
        [part(0, 0) + near_top + joined_top, part(0, half) + near_low + joined_low], axis=0
    )


def paired():
    count = lax.axis_size("dp")
    return count > 2 and count % 2 == 0


def row_major(value):
    return with_layout_constraint(value, Layout(major_to_minor=(0, 1)))


def split_columns(rows):
    count = lax.axis_size("dp")
    if not paired():
        return rows, None
    width = rows.shape[1] // count
    core = lax.axis_index("dp") % 2

    def half(which):
        return row_major(
            jnp.concatenate(
                [
                    lax.dynamic_slice_in_dim(rows, (first + which) * width, width, 1)
                    for first in range(0, count, 2)
                ],
                axis=1,
            )
        )

    return half(core), half(1 - core)


def weight_sums(pairs):
    keeps = []
    for (keep_rows, send_rows), right in pairs:
        if send_rows is None:
            keeps.append(narrow(contract(keep_rows, right, 0, 0)))
            continue
        sent = narrow(contract(send_rows, right, 0, 0))
        count = lax.axis_size("dp")
        got = lax.ppermute(sent, "dp", shift_pairs(count, 1))
        keeps.append(narrow(contract(keep_rows, right, 0, 0) + got.astype(jnp.float32)))
    return row_major(jnp.concatenate(keeps, axis=1))


def sum_shards(partial):
    count = lax.axis_size("dp")
    groups = [list(range(core, count, 2)) for core in range(2)] if paired() else None
    summed = lax.psum_scatter(
        partial, "dp", scatter_dimension=0, tiled=True, axis_index_groups=groups
    )
    return summed.astype(jnp.float32)


def sum_everywhere(value):
    for axis in ("tensor", "dp"):
        count = lax.axis_size(axis)
        if count & (count - 1):
            value = lax.psum(value, axis)
            continue
        step = 1
        while step < count:
            value = value + lax.ppermute(value, axis, shift_pairs(count, step))
            step *= 2
    return value


def product(left, right):
    return jnp.dot(left, right, preferred_element_type=jnp.float32)


def contract(left, right, left_axis, right_axis):
    return lax.dot_general(
        left,
        right,
        (((left_axis,), (right_axis,)), ((), ())),
        preferred_element_type=jnp.float32,
    )


def ordered(*values):
    return lax.optimization_barrier(values)


def narrow(value):
    return value.astype(jnp.bfloat16)


def whole_block(
    inputs,
    doc_lengths,
    attn_gain,
    w_query,
    w_key,
    value_weight,
    w_output,
    mlp_gain,
    w_gate,
    w_up,
    w_down,
    out_grad,
):
    tensor_rank = lax.axis_index("tensor")
    own_rows = inputs.shape[0]
    total_rows = own_rows * lax.axis_size("tensor")
    query_cols, key_cols = w_query.shape[1], w_key.shape[1]
    joint = query_cols + 2 * key_cols
    document_segment, positions, valid_rows = layout(doc_lengths[0], total_rows)
    valid_own = lax.dynamic_slice_in_dim(valid_rows, tensor_rank * own_rows, own_rows, 0)[:, None]
    cosine, sine_part = rope_tables(positions, HEAD_SIZE)
    gains = jnp.pad(jnp.stack([attn_gain, mlp_gain], axis=1), ((0, 0), (0, 126)))
    packed = lax.all_gather(
        row_major(jnp.concatenate([w_query, w_key, value_weight, gains, w_output.T], axis=1)),
        "dp",
        axis=0,
        tiled=True,
    )
    full_joint = packed[:, :joint]
    gain_one = packed[:, joint].astype(jnp.float32)
    gain_two = packed[:, joint + 1].astype(jnp.float32)
    full_output = packed[:, joint + gains.shape[1] :]
    hidden_half = w_gate.shape[1] // 2
    down_turned = w_down.T
    halves = [
        lax.all_gather(
            row_major(
                jnp.concatenate([w_gate[:, part], w_up[:, part], down_turned[:, part]], axis=1)
            ),
            "dp",
            axis=0,
            tiled=True,
        )
        for part in (slice(0, hidden_half), slice(hidden_half, 2 * hidden_half))
    ]

    grad_out = out_grad.astype(jnp.float32)
    head_count = query_cols // HEAD_SIZE
    kv_heads = key_cols // HEAD_SIZE
    residual = inputs.astype(jnp.float32)
    scale_one, unit_one = rms_stats(residual)
    inputs_all = gather_rows(inputs, "tensor")
    grad_mlp_all = gather_rows(narrow(grad_out * valid_own), "tensor", relative=True)
    normed_one_all = row_major(narrow(rms_stats(inputs_all.astype(jnp.float32))[1] * gain_one))
    seg_row, seg_col = document_segment[None, :], document_segment[:, None]
    joint_turned = contract(full_joint, normed_one_all, 0, 1)
    rotated, attended, log_total = attend(
        joint_turned, cosine, sine_part, seg_row, seg_col, head_count, kv_heads, QBLK
    )
    attn_out = scatter_rows(narrow(contract(attended, full_output, 0, 1)), "tensor")
    hidden = residual + valid_own * attn_out
    scale_two, unit_two = rms_stats(hidden)
    normed_two_all = gather_rows(narrow(unit_two * gain_two), "tensor", relative=True)
    pair_cols = 2 * hidden_half
    normed_split, cotangent_split = split_columns(normed_two_all), split_columns(grad_mlp_all)
    normed_total = mlp_total = None
    weight_grads = []
    for number, weights in enumerate(halves):
        pair_weights, down_weights = weights[:, :pair_cols], weights[:, pair_cols:]
        pair_pre = product(normed_two_all, pair_weights)
        grad_act = product(grad_mlp_all, down_weights)
        activation, grad_pair = activation_both(pair_pre, grad_act)
        if number == 1:
            normed_total = narrow(normed_total + contract(grad_pair, pair_weights, 1, 1))
            grad_pair, activation, normed_total = ordered(grad_pair, activation, normed_total)
            grad_normed_two = scatter_rows(normed_total, "tensor", relative=True)
        partial = weight_sums(((normed_split, grad_pair), (cotangent_split, activation)))
        if number == 0:
            grad_pair, activation, partial = ordered(grad_pair, activation, partial)
            normed_total = contract(grad_pair, pair_weights, 1, 1)
            mlp_total = contract(activation, down_weights, 1, 1)
            normed_two_all, grad_mlp_all, partial, normed_total, mlp_total = ordered(
                normed_two_all, grad_mlp_all, partial, normed_total, mlp_total
            )
        weight_grads.append(sum_shards(partial))
    mlp_gain_part = jnp.sum(grad_normed_two * unit_two, axis=0)
    grad_hidden = grad_out + norm_backward(grad_normed_two, unit_two, scale_two, gain_two)
    grad_attn = narrow(grad_hidden * valid_own)
    activation, grad_attn = ordered(activation, grad_attn)
    grad_attn_all = gather_rows(grad_attn, "tensor")
    mlp_part = narrow(mlp_total + contract(activation, down_weights, 1, 1))
    grad_attn_all, mlp_part = ordered(grad_attn_all, mlp_part)
    mlp_out = scatter_rows(mlp_part, "tensor", relative=True)
    output = hidden + valid_own * mlp_out
    grad_attended = narrow(contract(full_output, grad_attn_all, 0, 1))
    joint_back = attend_back(
        rotated,
        attended,
        grad_attended,
        log_total,
        cosine,
        sine_part,
        seg_row,
        seg_col,
        head_count,
        kv_heads,
        QBLK,
    )
    last_part = narrow(contract(joint_back, full_joint, 0, 1))
    joint_back, last_part = ordered(joint_back, last_part)
    grad_normed_one = scatter_rows(last_part, "tensor")
    tail = weight_sums(
        (
            (split_columns(normed_one_all), joint_back.T),
            (split_columns(grad_attn_all), attended.T),
        ),
    )
    tail_grad = sum_shards(tail)
    attn_gain_part = jnp.sum(grad_normed_one * unit_one, axis=0)
    input_grad = grad_hidden + norm_backward(grad_normed_one, unit_one, scale_one, gain_one)
    gain_sums = sum_everywhere(jnp.stack([attn_gain_part, mlp_gain_part]))
    gain_rows = attn_gain.shape[0]
    gain_own = lax.dynamic_slice_in_dim(gain_sums, lax.axis_index("dp") * gain_rows, gain_rows, 1)
    return (
        output,
        input_grad,
        gain_own[0],
        tail_grad[:, :query_cols],
        tail_grad[:, query_cols : query_cols + key_cols],
        tail_grad[:, query_cols + key_cols : joint],
        tail_grad[:, joint:].T,
        gain_own[1],
        jnp.concatenate([half[:, :hidden_half] for half in weight_grads], axis=1),
        jnp.concatenate([half[:, hidden_half:pair_cols] for half in weight_grads], axis=1),
        jnp.concatenate([half[:, pair_cols:].T for half in weight_grads], axis=0),
    )


def solution(mesh):
    placed = (
        P(("dp", "tensor"), None),
        P("dp", None),
        P("dp"),
        P("dp", "tensor"),
        P("dp", "tensor"),
        P("dp", "tensor"),
        P("tensor", "dp"),
        P("dp"),
        P("dp", "tensor"),
        P("dp", "tensor"),
        P("tensor", "dp"),
        P(("dp", "tensor"), None),
    )
    return jax.shard_map(
        whole_block,
        mesh=mesh,
        in_specs=placed,
        out_specs=(
            P(("dp", "tensor"), None),
            P(("dp", "tensor"), None),
            P("dp"),
            P("dp", "tensor"),
            P("dp", "tensor"),
            P("dp", "tensor"),
            P("tensor", "dp"),
            P("dp"),
            P("dp", "tensor"),
            P("dp", "tensor"),
            P("tensor", "dp"),
        ),
        check_vma=False,
    )
```

```python
import functools

import jax
import jax.numpy as jnp
from jax import lax
from jax.experimental import pallas as pl
from jax.experimental.layout import Layout, with_layout_constraint
from jax.experimental.pallas import tpu as pltpu
from jax.sharding import PartitionSpec as P


HEAD_SIZE = 64
QBLK = 256


epsilon = 1e-05
rope_base = 500000.0


def layout(lengths, total_rows):
    row_index = jnp.arange(total_rows, dtype=jnp.int32)
    doc_ends = jnp.cumsum(lengths)
    passed = doc_ends[None, :] <= row_index[:, None]
    document_segment = jnp.sum(passed.astype(jnp.int32), axis=1)
    doc_start = jnp.sum(jnp.where(passed, lengths[None, :], 0), axis=1)
    positions = (row_index - doc_start).astype(jnp.float32)
    valid_rows = (document_segment < lengths.shape[0]).astype(jnp.float32)
    return (document_segment, positions, valid_rows)


def rope_tables(positions, head_dim):
    half_dim = head_dim // 2
    inverse_freq = rope_base ** (-(jnp.arange(half_dim, dtype=jnp.float32) * 2.0 / head_dim))
    angles = positions[None, :] * inverse_freq[:, None]
    return (jnp.cos(angles), jnp.sin(angles))


def rms_stats(hidden):
    scale_row = lax.rsqrt(jnp.mean(hidden * hidden, axis=-1, keepdims=True) + epsilon)
    return (scale_row, hidden * scale_row)


def norm_backward(grad_normed, unit_rows, scale_row, gain_wide):
    scaled = grad_normed * gain_wide
    return scale_row * (scaled - unit_rows * jnp.mean(scaled * unit_rows, axis=-1, keepdims=True))


def rope_rows(ref, base, cosine, sine_part):
    half = HEAD_SIZE // 2
    first = ref[pl.ds(base, half), :]
    second = ref[pl.ds(base + half, half), :]
    return first * cosine - second * sine_part, second * cosine + first * sine_part


def fill_bias(bias_ref, seg_row_ref, seg_col_ref, start, block):
    keys = start + block
    key_index = lax.broadcasted_iota(jnp.int32, (keys, block), 0)
    query_index = lax.broadcasted_iota(jnp.int32, (keys, block), 1) + start
    allowed = (seg_col_ref[:keys, :] == seg_row_ref[:, start : start + block]) & (
        key_index <= query_index
    )
    bias_ref[:keys, :] = jnp.where(allowed, 0.0, -jnp.inf)


def head_base(index):
    return pl.multiple_of(index * HEAD_SIZE, HEAD_SIZE)


def turned(value):
    return jnp.transpose(value.astype(jnp.float32)).astype(jnp.bfloat16)


def attend_kernel(
    heads, kv_heads, block, joint_ref, cos_ref, sin_ref, seg_row_ref, seg_col_ref,
    rot_ref, att_ref, log_ref, krow_ref, bias_ref,
):
    rows = joint_ref.shape[1]
    half = HEAD_SIZE // 2
    group = heads // kv_heads
    value_base = (heads + kv_heads) * HEAD_SIZE

    def rotate_head(index, scale):
        base = head_base(index)
        first, second = rope_rows(joint_ref, base, cos_ref[...], sin_ref[...])
        rot_ref[pl.ds(base, half), :] = (first * scale).astype(jnp.bfloat16)
        rot_ref[pl.ds(base + half, half), :] = (second * scale).astype(jnp.bfloat16)

    @pl.loop(0, heads)
    def _(index):
        rotate_head(index, HEAD_SIZE ** (-0.5))

    @pl.loop(0, kv_heads)
    def _(index):
        rotate_head(heads + index, 1.0)
        krow_ref[index] = turned(rot_ref[pl.ds(head_base(heads + index), HEAD_SIZE), :])

    rot_ref[value_base:, :] = joint_ref[value_base:, :].astype(jnp.bfloat16)
    for start in range(0, rows, block):
        keys = start + block
        fill_bias(bias_ref, seg_row_ref, seg_col_ref, start, block)

        @pl.loop(0, heads)
        def _(head):
            kv_head = head // group
            query = rot_ref[pl.ds(head_base(head), HEAD_SIZE), start:keys]
            scores = (
                jnp.dot(krow_ref[kv_head, :keys, :], query, preferred_element_type=jnp.float32)
                + bias_ref[:keys, :]
            )
            top = jnp.max(scores, axis=0, keepdims=True)
            powers = jnp.exp(scores - top)
            total = jnp.sum(powers, axis=0, keepdims=True)
            weights = (powers * (1.0 / total)).astype(jnp.bfloat16)
            value = rot_ref[pl.ds(head_base(heads + kv_heads + kv_head), HEAD_SIZE), :keys]
            att_ref[pl.ds(head_base(head), HEAD_SIZE), start:keys] = jnp.dot(
                value, weights, preferred_element_type=jnp.float32
            ).astype(jnp.bfloat16)
            log_ref[pl.ds(head, 1), start:keys] = top + jnp.log(total)


def attend_back_kernel(
    heads, kv_heads, block, rot_ref, att_ref, out_ref, log_ref, cos_ref, sin_ref,
    seg_row_ref, seg_col_ref, back_ref, krow_ref, vrow_ref, dkey_ref, dvalue_ref, bias_ref,
):
    rows = rot_ref.shape[1]
    half = HEAD_SIZE // 2
    group = heads // kv_heads
    last = (((1,), (1,)), ((), ()))

    def turn_back(first, second, base, start, stop):
        cosine, sine_part = cos_ref[:, start:stop], sin_ref[:, start:stop]
        back_ref[pl.ds(base, half), start:stop] = (
            first * cosine + second * sine_part
        ).astype(jnp.bfloat16)
        back_ref[pl.ds(base + half, half), start:stop] = (
            second * cosine - first * sine_part
        ).astype(jnp.bfloat16)

    @pl.loop(0, kv_heads)
    def _(index):
        krow_ref[index] = turned(rot_ref[pl.ds(head_base(heads + index), HEAD_SIZE), :])
        vrow_ref[index] = turned(rot_ref[pl.ds(head_base(heads + kv_heads + index), HEAD_SIZE), :])

    dkey_ref[...] = jnp.zeros_like(dkey_ref)
    dvalue_ref[...] = jnp.zeros_like(dvalue_ref)
    for start in range(0, rows, block):
        keys = start + block
        fill_bias(bias_ref, seg_row_ref, seg_col_ref, start, block)

        @pl.loop(0, heads)
        def _(head):
            kv_head = head // group
            own = pl.ds(head_base(head), HEAD_SIZE)
            query = rot_ref[own, start:keys]
            grad = out_ref[own, start:keys]
            delta = jnp.sum(
                grad.astype(jnp.float32) * att_ref[own, start:keys].astype(jnp.float32),
                axis=0,
                keepdims=True,
            )
            scores = (
                jnp.dot(krow_ref[kv_head, :keys, :], query, preferred_element_type=jnp.float32)
                + bias_ref[:keys, :]
            )
            probs = jnp.exp(scores - log_ref[pl.ds(head, 1), start:keys])
            grad_probs = jnp.dot(
                vrow_ref[kv_head, :keys, :], grad, preferred_element_type=jnp.float32
            )
            grad_scores = (probs * (grad_probs - delta)).astype(jnp.bfloat16)
            dvalue_ref[kv_head, :keys, :] += lax.dot_general(
                probs.astype(jnp.bfloat16), grad, last, preferred_element_type=jnp.float32
            )
            dkey_ref[kv_head, :keys, :] += lax.dot_general(
                grad_scores, query, last, preferred_element_type=jnp.float32
            )
            key = rot_ref[pl.ds(head_base(heads + kv_head), HEAD_SIZE), :keys]
            dquery = jnp.dot(key, grad_scores, preferred_element_type=jnp.float32) * (
                HEAD_SIZE ** (-0.5)
            )
            turn_back(dquery[:half], dquery[half:], head_base(head), start, keys)

    @pl.loop(0, kv_heads)
    def _(index):
        dkey = jnp.transpose(dkey_ref[index])
        turn_back(dkey[:half], dkey[half:], head_base(heads + index), 0, rows)
        back_ref[pl.ds(head_base(heads + kv_heads + index), HEAD_SIZE), :] = jnp.transpose(
            dvalue_ref[index]
        ).astype(jnp.bfloat16)


def activation_kernel(pair_ref, grad_ref, act_ref, out_ref):
    units = grad_ref.shape[1]
    gate, up = pair_ref[:, :units], pair_ref[:, units:]
    grad = grad_ref[...]
    sigmoid_gate = 1.0 / (1.0 + jnp.exp(-gate))
    act_ref[...] = (gate * sigmoid_gate * up).astype(jnp.bfloat16)
    grad_gate = grad * up * sigmoid_gate * (1.0 + gate * (1.0 - sigmoid_gate))
    out_ref[:, :units] = grad_gate.astype(jnp.bfloat16)
    out_ref[:, units:] = (grad * gate * sigmoid_gate).astype(jnp.bfloat16)


def activation_both(pair, grad):
    rows, units = grad.shape
    block = min(rows, 256)

    def at(row):
        return (row, 0)

    return pl.pallas_call(
        activation_kernel,
        out_shape=(
            jax.ShapeDtypeStruct(grad.shape, jnp.bfloat16),
            jax.ShapeDtypeStruct(pair.shape, jnp.bfloat16),
        ),
        grid=(rows // block,),
        in_specs=[pl.BlockSpec((block, 2 * units), at), pl.BlockSpec((block, units), at)],
        out_specs=(pl.BlockSpec((block, units), at), pl.BlockSpec((block, 2 * units), at)),
        cost_estimate=pl.CostEstimate(
            flops=20 * pair.size, bytes_accessed=9 * pair.size, transcendentals=pair.size
        ),
        name="activation_both",
    )(pair, grad)


def in_vmem(count):
    return [pl.BlockSpec(memory_space=pltpu.VMEM)] * count


def attend(joint, cosine, sine_part, seg_row, seg_col, heads, kv_heads, block):
    rows = joint.shape[1]
    flops = 2 * heads * rows * rows * HEAD_SIZE
    return pl.pallas_call(
        functools.partial(attend_kernel, heads, kv_heads, block),
        out_shape=(
            jax.ShapeDtypeStruct(joint.shape, jnp.bfloat16),
            jax.ShapeDtypeStruct((heads * HEAD_SIZE, rows), jnp.bfloat16),
            jax.ShapeDtypeStruct((heads, rows), jnp.float32),
        ),
        in_specs=in_vmem(5),
        out_specs=tuple(in_vmem(3)),
        scratch_shapes=[
            pltpu.VMEM((kv_heads, rows, HEAD_SIZE), jnp.bfloat16),
            pltpu.VMEM((rows, block), jnp.float32),
        ],
        cost_estimate=pl.CostEstimate(
            flops=8 * flops, bytes_accessed=8 * joint.size, transcendentals=heads * rows * rows
        ),
        name="attend",
    )(joint, cosine, sine_part, seg_row, seg_col)


def attend_back(rotated, attended, grad, log_total, cosine, sine_part, seg_row, seg_col, heads, kv_heads, block):
    rows = rotated.shape[1]
    flops = 2 * heads * rows * rows * HEAD_SIZE
    return pl.pallas_call(
        functools.partial(attend_back_kernel, heads, kv_heads, block),
        out_shape=jax.ShapeDtypeStruct(rotated.shape, jnp.bfloat16),
        in_specs=in_vmem(8),
        out_specs=pl.BlockSpec(memory_space=pltpu.VMEM),
        scratch_shapes=[
            pltpu.VMEM((kv_heads, rows, HEAD_SIZE), jnp.bfloat16),
            pltpu.VMEM((kv_heads, rows, HEAD_SIZE), jnp.bfloat16),
            pltpu.VMEM((kv_heads, rows, HEAD_SIZE), jnp.float32),
            pltpu.VMEM((kv_heads, rows, HEAD_SIZE), jnp.float32),
            pltpu.VMEM((rows, block), jnp.float32),
        ],
        cost_estimate=pl.CostEstimate(
            flops=20 * flops, bytes_accessed=8 * rotated.size, transcendentals=heads * rows * rows
        ),
        name="attend_back",
    )(rotated, attended, grad, log_total, cosine, sine_part, seg_row, seg_col)


def shift_pairs(count, mask):
    return [(i, i ^ mask) for i in range(count)]


def gather_rows(block, axis, relative=False):
    count = lax.axis_size(axis)
    if count != 4:
        return lax.all_gather(block, axis, axis=0, tiled=True)
    me = lax.axis_index(axis)
    rows = block.shape[0]
    half = rows // 2
    from_x = lax.ppermute(block, axis, shift_pairs(count, 1))
    from_y = lax.ppermute(block, axis, shift_pairs(count, 2))
    far_top = lax.ppermute(from_x[:half], axis, shift_pairs(count, 2))
    far_low = lax.ppermute(from_y[half:], axis, shift_pairs(count, 1))
    if relative:
        return jnp.concatenate([block, from_x, from_y, far_top, far_low], axis=0)
    whole = jnp.zeros((count * rows, block.shape[1]), block.dtype)
    for mask, piece, extra in (
        (0, block, 0),
        (1, from_x, 0),
        (2, from_y, 0),
        (3, far_top, 0),
        (3, far_low, half),
    ):
        whole = lax.dynamic_update_slice(whole, piece, ((me ^ mask) * rows + extra, 0))
    return row_major(whole)


def scatter_rows(partial, axis, relative=False):
    count = lax.axis_size(axis)
    if count != 4:
        return lax.psum_scatter(partial, axis, scatter_dimension=0, tiled=True).astype(jnp.float32)
    me = 0 if relative else lax.axis_index(axis)
    rows = partial.shape[0] // count
    half = rows // 2

    def part(mask, extra):
        return lax.dynamic_slice_in_dim(partial, (me ^ mask) * rows + extra, half, 0)

    def send(piece, mask):
        return lax.ppermute(piece, axis, shift_pairs(count, mask))

    relay_top = send(part(3, 0), 1).astype(jnp.float32)
    relay_low = send(part(3, half), 2).astype(jnp.float32)
    near_top = send(part(1, 0), 1).astype(jnp.float32)
    near_low = send(part(2, half), 2).astype(jnp.float32)
    joined_top = send(narrow(part(2, 0) + relay_top), 2).astype(jnp.float32)
    joined_low = send(narrow(part(1, half) + relay_low), 1).astype(jnp.float32)
    return jnp.concatenate(
        [part(0, 0) + near_top + joined_top, part(0, half) + near_low + joined_low], axis=0
    )


def paired():
    count = lax.axis_size("dp")
    return count > 2 and count % 2 == 0


def row_major(value):
    return with_layout_constraint(value, Layout(major_to_minor=(0, 1)))


def split_columns(rows):
    count = lax.axis_size("dp")
    if not paired():
        return rows, None
    width = rows.shape[1] // count
    core = lax.axis_index("dp") % 2

    def half(which):
        return row_major(
            jnp.concatenate(
                [
                    lax.dynamic_slice_in_dim(rows, (first + which) * width, width, 1)
                    for first in range(0, count, 2)
                ],
                axis=1,
            )
        )

    return half(core), half(1 - core)


def weight_sums(pairs):
    keeps = []
    for (keep_rows, send_rows), right in pairs:
        if send_rows is None:
            keeps.append(narrow(contract(keep_rows, right, 0, 0)))
            continue
        sent = narrow(contract(send_rows, right, 0, 0))
        count = lax.axis_size("dp")
        got = lax.ppermute(sent, "dp", shift_pairs(count, 1))
        keeps.append(narrow(contract(keep_rows, right, 0, 0) + got.astype(jnp.float32)))
    return row_major(jnp.concatenate(keeps, axis=1))


def sum_shards(partial):
    count = lax.axis_size("dp")
    groups = [list(range(core, count, 2)) for core in range(2)] if paired() else None
    summed = lax.psum_scatter(
        partial, "dp", scatter_dimension=0, tiled=True, axis_index_groups=groups
    )
    return summed.astype(jnp.float32)


def sum_everywhere(value, axes):
    for axis in axes:
        count = lax.axis_size(axis)
        if count & (count - 1):
            value = lax.psum(value, axis)
            continue
        step = 1
        while step < count:
            value = value + lax.ppermute(value, axis, shift_pairs(count, step))
            step *= 2
    return value


def product(left, right):
    return jnp.dot(left, right, preferred_element_type=jnp.float32)


def contract(left, right, left_axis, right_axis):
    return lax.dot_general(
        left,
        right,
        (((left_axis,), (right_axis,)), ((), ())),
        preferred_element_type=jnp.float32,
    )


def ordered(*values):
    return lax.optimization_barrier(values)


def narrow(value):
    return value.astype(jnp.bfloat16)


def whole_block(
    inputs,
    doc_lengths,
    attn_gain,
    w_query,
    w_key,
    value_weight,
    w_output,
    mlp_gain,
    w_gate,
    w_up,
    w_down,
    out_grad,
):
    tensor_rank = lax.axis_index("tensor")
    own_rows = inputs.shape[0]
    total_rows = own_rows * lax.axis_size("tensor")
    query_cols, key_cols = w_query.shape[1], w_key.shape[1]
    joint = query_cols + 2 * key_cols
    document_segment, positions, valid_rows = layout(doc_lengths[0], total_rows)
    valid_own = lax.dynamic_slice_in_dim(valid_rows, tensor_rank * own_rows, own_rows, 0)[:, None]
    cosine, sine_part = rope_tables(positions, HEAD_SIZE)
    gain_rows = attn_gain.shape[0]
    gains = sum_everywhere(
        lax.dynamic_update_slice(
            jnp.zeros((2, inputs.shape[1]), jnp.float32),
            jnp.stack([attn_gain, mlp_gain]).astype(jnp.float32),
            (0, lax.axis_index("dp") * gain_rows),
        ),
        ("dp",),
    )
    gain_one, gain_two = gains[0], gains[1]
    packed = lax.all_gather(
        row_major(jnp.concatenate([w_query, w_key, value_weight, w_output.T], axis=1)),
        "dp",
        axis=0,
        tiled=True,
    )
    full_joint = packed[:, :joint]
    full_output = packed[:, joint:]
    hidden_units = w_gate.shape[1]
    cut = max(128, hidden_units * 5 // 8 // 128 * 128)
    down_turned = w_down.T
    halves = [
        lax.all_gather(
            row_major(
                jnp.concatenate([w_gate[:, part], w_up[:, part], down_turned[:, part]], axis=1)
            ),
            "dp",
            axis=0,
            tiled=True,
        )
        for part in (slice(0, cut), slice(cut, hidden_units))
    ]

    grad_out = out_grad.astype(jnp.float32)
    head_count = query_cols // HEAD_SIZE
    kv_heads = key_cols // HEAD_SIZE
    residual = inputs.astype(jnp.float32)
    scale_one, unit_one = rms_stats(residual)
    inputs_all = gather_rows(inputs, "tensor")
    grad_mlp_all = gather_rows(narrow(grad_out * valid_own), "tensor", relative=True)
    normed_one_all = row_major(narrow(rms_stats(inputs_all.astype(jnp.float32))[1] * gain_one))
    seg_row, seg_col = document_segment[None, :], document_segment[:, None]
    joint_turned = contract(full_joint, normed_one_all, 0, 1)
    rotated, attended, log_total = attend(
        joint_turned, cosine, sine_part, seg_row, seg_col, head_count, kv_heads, QBLK
    )
    attn_out = scatter_rows(narrow(contract(attended, full_output, 0, 1)), "tensor")
    hidden = residual + valid_own * attn_out
    scale_two, unit_two = rms_stats(hidden)
    normed_two_all = gather_rows(narrow(unit_two * gain_two), "tensor", relative=True)
    normed_split, cotangent_split = split_columns(normed_two_all), split_columns(grad_mlp_all)
    normed_total = mlp_total = None
    weight_grads = []
    for number, weights in enumerate(halves):
        pair_cols = 2 * (weights.shape[1] // 3)
        pair_weights, down_weights = weights[:, :pair_cols], weights[:, pair_cols:]
        pair_pre = product(normed_two_all, pair_weights)
        grad_act = product(grad_mlp_all, down_weights)
        activation, grad_pair = activation_both(pair_pre, grad_act)
        if number == 1:
            normed_total = narrow(contract(grad_pair, pair_weights, 1, 1) + normed_total.astype(jnp.float32))
            grad_pair, activation, normed_total = ordered(grad_pair, activation, normed_total)
            grad_normed_two = scatter_rows(normed_total, "tensor", relative=True)
        partial = weight_sums(((normed_split, grad_pair), (cotangent_split, activation)))
        if number == 0:
            grad_pair, activation, partial = ordered(grad_pair, activation, partial)
            normed_total = narrow(contract(grad_pair, pair_weights, 1, 1))
            mlp_total = narrow(contract(activation, down_weights, 1, 1))
            normed_two_all, grad_mlp_all, partial, normed_total, mlp_total = ordered(
                normed_two_all, grad_mlp_all, partial, normed_total, mlp_total
            )
        weight_grads.append(sum_shards(partial))
    mlp_gain_part = jnp.sum(grad_normed_two * unit_two, axis=0)
    grad_hidden = grad_out + norm_backward(grad_normed_two, unit_two, scale_two, gain_two)
    grad_attn = narrow(grad_hidden * valid_own)
    activation, grad_attn = ordered(activation, grad_attn)
    grad_attn_all = gather_rows(grad_attn, "tensor")
    mlp_part = narrow(contract(activation, down_weights, 1, 1) + mlp_total.astype(jnp.float32))
    grad_attn_all, mlp_part = ordered(grad_attn_all, mlp_part)
    mlp_out = scatter_rows(mlp_part, "tensor", relative=True)
    output = hidden + valid_own * mlp_out
    grad_attended = narrow(contract(full_output, grad_attn_all, 0, 1))
    joint_back = attend_back(
        rotated,
        attended,
        grad_attended,
        log_total,
        cosine,
        sine_part,
        seg_row,
        seg_col,
        head_count,
        kv_heads,
        QBLK,
    )
    tail = weight_sums(
        (
            (split_columns(normed_one_all), joint_back.T),
            (split_columns(grad_attn_all), attended.T),
        ),
    )
    tail_grad = sum_shards(tail)
    last_part = narrow(contract(joint_back, full_joint, 0, 1))
    grad_normed_one = scatter_rows(last_part, "tensor")
    attn_gain_part = jnp.sum(grad_normed_one * unit_one, axis=0)
    input_grad = grad_hidden + norm_backward(grad_normed_one, unit_one, scale_one, gain_one)
    gain_sums = sum_everywhere(jnp.stack([attn_gain_part, mlp_gain_part]), ("tensor", "dp"))
    gain_own = lax.dynamic_slice_in_dim(gain_sums, lax.axis_index("dp") * gain_rows, gain_rows, 1)
    return (
        output,
        input_grad,
        gain_own[0],
        tail_grad[:, :query_cols],
        tail_grad[:, query_cols : query_cols + key_cols],
        tail_grad[:, query_cols + key_cols : joint],
        tail_grad[:, joint:].T,
        gain_own[1],
        jnp.concatenate([part[:, : part.shape[1] // 3] for part in weight_grads], axis=1),
        jnp.concatenate(
            [part[:, part.shape[1] // 3 : 2 * (part.shape[1] // 3)] for part in weight_grads],
            axis=1,
        ),
        jnp.concatenate(
            [part[:, 2 * (part.shape[1] // 3) :].T for part in weight_grads], axis=0
        ),
    )


def solution(mesh):
    placed = (
        P(("dp", "tensor"), None),
        P("dp", None),
        P("dp"),
        P("dp", "tensor"),
        P("dp", "tensor"),
        P("dp", "tensor"),
        P("tensor", "dp"),
        P("dp"),
        P("dp", "tensor"),
        P("dp", "tensor"),
        P("tensor", "dp"),
        P(("dp", "tensor"), None),
    )
    return jax.shard_map(
        whole_block,
        mesh=mesh,
        in_specs=placed,
        out_specs=(
            P(("dp", "tensor"), None),
            P(("dp", "tensor"), None),
            P("dp"),
            P("dp", "tensor"),
            P("dp", "tensor"),
            P("dp", "tensor"),
            P("tensor", "dp"),
            P("dp"),
            P("dp", "tensor"),
            P("dp", "tensor"),
            P("tensor", "dp"),
        ),
        check_vma=False,
    )
```

```python
import functools

import jax
import jax.numpy as jnp
from jax import lax
from jax.experimental import pallas as pl
from jax.experimental.layout import Layout, with_layout_constraint
from jax.experimental.pallas import tpu as pltpu
from jax.sharding import PartitionSpec as P


HEAD_SIZE = 64
QBLK = 256


epsilon = 1e-05
rope_base = 500000.0


def layout(lengths, total_rows):
    row_index = jnp.arange(total_rows, dtype=jnp.int32)
    doc_ends = jnp.cumsum(lengths)
    passed = doc_ends[None, :] <= row_index[:, None]
    document_segment = jnp.sum(passed.astype(jnp.int32), axis=1)
    doc_start = jnp.sum(jnp.where(passed, lengths[None, :], 0), axis=1)
    positions = (row_index - doc_start).astype(jnp.float32)
    valid_rows = (document_segment < lengths.shape[0]).astype(jnp.float32)
    return (document_segment, positions, valid_rows)


def rope_tables(positions, head_dim):
    half_dim = head_dim // 2
    inverse_freq = rope_base ** (-(jnp.arange(half_dim, dtype=jnp.float32) * 2.0 / head_dim))
    angles = positions[None, :] * inverse_freq[:, None]
    return (jnp.cos(angles), jnp.sin(angles))


def rms_stats(hidden):
    scale_row = lax.rsqrt(jnp.mean(hidden * hidden, axis=-1, keepdims=True) + epsilon)
    return (scale_row, hidden * scale_row)


def norm_backward(grad_normed, unit_rows, scale_row, gain_wide):
    scaled = grad_normed * gain_wide
    return scale_row * (scaled - unit_rows * jnp.mean(scaled * unit_rows, axis=-1, keepdims=True))


def rope_rows(ref, base, cosine, sine_part):
    half = HEAD_SIZE // 2
    first = ref[pl.ds(base, half), :]
    second = ref[pl.ds(base + half, half), :]
    return first * cosine - second * sine_part, second * cosine + first * sine_part


def fill_bias(bias_ref, seg_row_ref, seg_col_ref, start, block):
    keys = start + block
    key_index = lax.broadcasted_iota(jnp.int32, (keys, block), 0)
    query_index = lax.broadcasted_iota(jnp.int32, (keys, block), 1) + start
    allowed = (seg_col_ref[:keys, :] == seg_row_ref[:, start : start + block]) & (
        key_index <= query_index
    )
    bias_ref[:keys, :] = jnp.where(allowed, 0.0, -jnp.inf)


def head_base(index):
    return pl.multiple_of(index * HEAD_SIZE, HEAD_SIZE)


def turned(value):
    return jnp.transpose(value.astype(jnp.float32)).astype(jnp.bfloat16)


def attend_kernel(
    heads, kv_heads, block, joint_ref, cos_ref, sin_ref, seg_row_ref, seg_col_ref,
    rot_ref, att_ref, log_ref, krow_ref, bias_ref,
):
    rows = joint_ref.shape[1]
    half = HEAD_SIZE // 2
    group = heads // kv_heads
    value_base = (heads + kv_heads) * HEAD_SIZE

    def rotate_head(index, scale):
        base = head_base(index)
        first, second = rope_rows(joint_ref, base, cos_ref[...], sin_ref[...])
        rot_ref[pl.ds(base, half), :] = (first * scale).astype(jnp.bfloat16)
        rot_ref[pl.ds(base + half, half), :] = (second * scale).astype(jnp.bfloat16)

    @pl.loop(0, heads)
    def _(index):
        rotate_head(index, HEAD_SIZE ** (-0.5))

    @pl.loop(0, kv_heads)
    def _(index):
        rotate_head(heads + index, 1.0)
        krow_ref[index] = turned(rot_ref[pl.ds(head_base(heads + index), HEAD_SIZE), :])

    rot_ref[value_base:, :] = joint_ref[value_base:, :].astype(jnp.bfloat16)
    for start in range(0, rows, block):
        keys = start + block
        fill_bias(bias_ref, seg_row_ref, seg_col_ref, start, block)

        @pl.loop(0, heads)
        def _(head):
            kv_head = head // group
            query = rot_ref[pl.ds(head_base(head), HEAD_SIZE), start:keys]
            scores = (
                jnp.dot(krow_ref[kv_head, :keys, :], query, preferred_element_type=jnp.float32)
                + bias_ref[:keys, :]
            )
            top = jnp.max(scores, axis=0, keepdims=True)
            powers = jnp.exp(scores - top)
            total = jnp.sum(powers, axis=0, keepdims=True)
            weights = (powers * (1.0 / total)).astype(jnp.bfloat16)
            value = rot_ref[pl.ds(head_base(heads + kv_heads + kv_head), HEAD_SIZE), :keys]
            att_ref[pl.ds(head_base(head), HEAD_SIZE), start:keys] = jnp.dot(
                value, weights, preferred_element_type=jnp.float32
            ).astype(jnp.bfloat16)
            log_ref[pl.ds(head, 1), start:keys] = top + jnp.log(total)


def attend_back_kernel(
    heads, kv_heads, block, rot_ref, att_ref, out_ref, log_ref, cos_ref, sin_ref,
    seg_row_ref, seg_col_ref, back_ref, krow_ref, vrow_ref, dkey_ref, dvalue_ref, bias_ref,
):
    rows = rot_ref.shape[1]
    half = HEAD_SIZE // 2
    group = heads // kv_heads
    last = (((1,), (1,)), ((), ()))

    def turn_back(first, second, base, start, stop):
        cosine, sine_part = cos_ref[:, start:stop], sin_ref[:, start:stop]
        back_ref[pl.ds(base, half), start:stop] = (
            first * cosine + second * sine_part
        ).astype(jnp.bfloat16)
        back_ref[pl.ds(base + half, half), start:stop] = (
            second * cosine - first * sine_part
        ).astype(jnp.bfloat16)

    @pl.loop(0, kv_heads)
    def _(index):
        krow_ref[index] = turned(rot_ref[pl.ds(head_base(heads + index), HEAD_SIZE), :])
        vrow_ref[index] = turned(rot_ref[pl.ds(head_base(heads + kv_heads + index), HEAD_SIZE), :])

    dkey_ref[...] = jnp.zeros_like(dkey_ref)
    dvalue_ref[...] = jnp.zeros_like(dvalue_ref)
    for start in range(0, rows, block):
        keys = start + block
        fill_bias(bias_ref, seg_row_ref, seg_col_ref, start, block)

        @pl.loop(0, heads)
        def _(head):
            kv_head = head // group
            own = pl.ds(head_base(head), HEAD_SIZE)
            query = rot_ref[own, start:keys]
            grad = out_ref[own, start:keys]
            delta = jnp.sum(
                grad.astype(jnp.float32) * att_ref[own, start:keys].astype(jnp.float32),
                axis=0,
                keepdims=True,
            )
            scores = (
                jnp.dot(krow_ref[kv_head, :keys, :], query, preferred_element_type=jnp.float32)
                + bias_ref[:keys, :]
            )
            probs = jnp.exp(scores - log_ref[pl.ds(head, 1), start:keys])
            grad_probs = jnp.dot(
                vrow_ref[kv_head, :keys, :], grad, preferred_element_type=jnp.float32
            )
            grad_scores = (probs * (grad_probs - delta)).astype(jnp.bfloat16)
            dvalue_ref[kv_head, :keys, :] += lax.dot_general(
                probs.astype(jnp.bfloat16), grad, last, preferred_element_type=jnp.float32
            )
            dkey_ref[kv_head, :keys, :] += lax.dot_general(
                grad_scores, query, last, preferred_element_type=jnp.float32
            )
            key = rot_ref[pl.ds(head_base(heads + kv_head), HEAD_SIZE), :keys]
            dquery = jnp.dot(key, grad_scores, preferred_element_type=jnp.float32) * (
                HEAD_SIZE ** (-0.5)
            )
            turn_back(dquery[:half], dquery[half:], head_base(head), start, keys)

    @pl.loop(0, kv_heads)
    def _(index):
        dkey = jnp.transpose(dkey_ref[index])
        turn_back(dkey[:half], dkey[half:], head_base(heads + index), 0, rows)
        back_ref[pl.ds(head_base(heads + kv_heads + index), HEAD_SIZE), :] = jnp.transpose(
            dvalue_ref[index]
        ).astype(jnp.bfloat16)


def activation_kernel(pair_ref, grad_ref, act_ref, out_ref):
    units = grad_ref.shape[1]
    gate, up = pair_ref[:, :units], pair_ref[:, units:]
    grad = grad_ref[...]
    sigmoid_gate = 1.0 / (1.0 + jnp.exp(-gate))
    act_ref[...] = (gate * sigmoid_gate * up).astype(jnp.bfloat16)
    grad_gate = grad * up * sigmoid_gate * (1.0 + gate * (1.0 - sigmoid_gate))
    out_ref[:, :units] = grad_gate.astype(jnp.bfloat16)
    out_ref[:, units:] = (grad * gate * sigmoid_gate).astype(jnp.bfloat16)


def activation_both(pair, grad):
    rows, units = grad.shape
    block = min(rows, 256)

    def at(row):
        return (row, 0)

    return pl.pallas_call(
        activation_kernel,
        out_shape=(
            jax.ShapeDtypeStruct(grad.shape, jnp.bfloat16),
            jax.ShapeDtypeStruct(pair.shape, jnp.bfloat16),
        ),
        grid=(rows // block,),
        in_specs=[pl.BlockSpec((block, 2 * units), at), pl.BlockSpec((block, units), at)],
        out_specs=(pl.BlockSpec((block, units), at), pl.BlockSpec((block, 2 * units), at)),
        cost_estimate=pl.CostEstimate(
            flops=20 * pair.size, bytes_accessed=9 * pair.size, transcendentals=pair.size
        ),
        name="activation_both",
    )(pair, grad)


def in_vmem(count):
    return [pl.BlockSpec(memory_space=pltpu.VMEM)] * count


def attend(joint, cosine, sine_part, seg_row, seg_col, heads, kv_heads, block):
    rows = joint.shape[1]
    flops = 2 * heads * rows * rows * HEAD_SIZE
    return pl.pallas_call(
        functools.partial(attend_kernel, heads, kv_heads, block),
        out_shape=(
            jax.ShapeDtypeStruct(joint.shape, jnp.bfloat16),
            jax.ShapeDtypeStruct((heads * HEAD_SIZE, rows), jnp.bfloat16),
            jax.ShapeDtypeStruct((heads, rows), jnp.float32),
        ),
        in_specs=in_vmem(5),
        out_specs=tuple(in_vmem(3)),
        scratch_shapes=[
            pltpu.VMEM((kv_heads, rows, HEAD_SIZE), jnp.bfloat16),
            pltpu.VMEM((rows, block), jnp.float32),
        ],
        cost_estimate=pl.CostEstimate(
            flops=8 * flops, bytes_accessed=8 * joint.size, transcendentals=heads * rows * rows
        ),
        name="attend",
    )(joint, cosine, sine_part, seg_row, seg_col)


def attend_back(rotated, attended, grad, log_total, cosine, sine_part, seg_row, seg_col, heads, kv_heads, block):
    rows = rotated.shape[1]
    flops = 2 * heads * rows * rows * HEAD_SIZE
    return pl.pallas_call(
        functools.partial(attend_back_kernel, heads, kv_heads, block),
        out_shape=jax.ShapeDtypeStruct(rotated.shape, jnp.bfloat16),
        in_specs=in_vmem(8),
        out_specs=pl.BlockSpec(memory_space=pltpu.VMEM),
        scratch_shapes=[
            pltpu.VMEM((kv_heads, rows, HEAD_SIZE), jnp.bfloat16),
            pltpu.VMEM((kv_heads, rows, HEAD_SIZE), jnp.bfloat16),
            pltpu.VMEM((kv_heads, rows, HEAD_SIZE), jnp.float32),
            pltpu.VMEM((kv_heads, rows, HEAD_SIZE), jnp.float32),
            pltpu.VMEM((rows, block), jnp.float32),
        ],
        cost_estimate=pl.CostEstimate(
            flops=20 * flops, bytes_accessed=8 * rotated.size, transcendentals=heads * rows * rows
        ),
        name="attend_back",
    )(rotated, attended, grad, log_total, cosine, sine_part, seg_row, seg_col)


def shift_pairs(count, mask):
    return [(i, i ^ mask) for i in range(count)]


def gather_rows(block, axis, relative=False):
    count = lax.axis_size(axis)
    if count != 4:
        return lax.all_gather(block, axis, axis=0, tiled=True)
    me = lax.axis_index(axis)
    rows = block.shape[0]
    half = rows // 2
    from_x = lax.ppermute(block, axis, shift_pairs(count, 1))
    from_y = lax.ppermute(block, axis, shift_pairs(count, 2))
    far_top = lax.ppermute(from_x[:half], axis, shift_pairs(count, 2))
    far_low = lax.ppermute(from_y[half:], axis, shift_pairs(count, 1))
    if relative:
        return jnp.concatenate([block, from_x, from_y, far_top, far_low], axis=0)
    whole = jnp.zeros((count * rows, block.shape[1]), block.dtype)
    for mask, piece, extra in (
        (0, block, 0),
        (1, from_x, 0),
        (2, from_y, 0),
        (3, far_top, 0),
        (3, far_low, half),
    ):
        whole = lax.dynamic_update_slice(whole, piece, ((me ^ mask) * rows + extra, 0))
    return row_major(whole)


def scatter_rows(partial, axis, relative=False):
    count = lax.axis_size(axis)
    if count != 4:
        return lax.psum_scatter(partial, axis, scatter_dimension=0, tiled=True).astype(jnp.float32)
    me = 0 if relative else lax.axis_index(axis)
    rows = partial.shape[0] // count
    half = rows // 2

    def part(mask, extra):
        return lax.dynamic_slice_in_dim(partial, (me ^ mask) * rows + extra, half, 0)

    def send(piece, mask):
        return lax.ppermute(piece, axis, shift_pairs(count, mask))

    relay_top = send(part(3, 0), 1).astype(jnp.float32)
    relay_low = send(part(3, half), 2).astype(jnp.float32)
    near_top = send(part(1, 0), 1).astype(jnp.float32)
    near_low = send(part(2, half), 2).astype(jnp.float32)
    top_sum, low_sum = ordered(narrow(part(2, 0) + relay_top), narrow(part(1, half) + relay_low))
    joined_top = send(top_sum, 2).astype(jnp.float32)
    joined_low = send(low_sum, 1).astype(jnp.float32)
    return jnp.concatenate(
        [part(0, 0) + near_top + joined_top, part(0, half) + near_low + joined_low], axis=0
    )


def scatter_direct(partial, axis):
    count = lax.axis_size(axis)
    if count != 4:
        return lax.psum_scatter(partial, axis, scatter_dimension=0, tiled=True).astype(jnp.float32)
    rows = partial.shape[0] // count
    total = partial[:rows].astype(jnp.float32)
    for mask in (3, 1, 2):
        piece = partial[mask * rows : (mask + 1) * rows]
        got = lax.ppermute(piece, axis, shift_pairs(count, mask))
        total = total + got.astype(jnp.float32)
    return total


def paired():
    count = lax.axis_size("dp")
    return count > 2 and count % 2 == 0


def row_major(value):
    return with_layout_constraint(value, Layout(major_to_minor=(0, 1)))


def split_columns(rows):
    count = lax.axis_size("dp")
    if not paired():
        return rows, None
    width = rows.shape[1] // count
    core = lax.axis_index("dp") % 2

    def half(which):
        return row_major(
            jnp.concatenate(
                [
                    lax.dynamic_slice_in_dim(rows, (first + which) * width, width, 1)
                    for first in range(0, count, 2)
                ],
                axis=1,
            )
        )

    return half(core), half(1 - core)


def weight_sums(pairs):
    keeps = []
    for (keep_rows, send_rows), right in pairs:
        if send_rows is None:
            keeps.append(narrow(contract(keep_rows, right, 0, 0)))
            continue
        sent = narrow(contract(send_rows, right, 0, 0))
        count = lax.axis_size("dp")
        got = lax.ppermute(sent, "dp", shift_pairs(count, 1))
        keeps.append(narrow(contract(keep_rows, right, 0, 0) + got.astype(jnp.float32)))
    return row_major(jnp.concatenate(keeps, axis=1))


def sum_shards(partial):
    count = lax.axis_size("dp")
    groups = [list(range(core, count, 2)) for core in range(2)] if paired() else None
    summed = lax.psum_scatter(
        partial, "dp", scatter_dimension=0, tiled=True, axis_index_groups=groups
    )
    return summed.astype(jnp.float32)


def sum_everywhere(value, axes):
    for axis in axes:
        count = lax.axis_size(axis)
        if count & (count - 1):
            value = lax.psum(value, axis)
            continue
        step = 1
        while step < count:
            value = value + lax.ppermute(value, axis, shift_pairs(count, step))
            step *= 2
    return value


def product(left, right):
    return jnp.dot(left, right, preferred_element_type=jnp.float32)


def contract(left, right, left_axis, right_axis):
    return lax.dot_general(
        left,
        right,
        (((left_axis,), (right_axis,)), ((), ())),
        preferred_element_type=jnp.float32,
    )


def ordered(*values):
    return lax.optimization_barrier(values)


def narrow(value):
    return value.astype(jnp.bfloat16)


def whole_block(
    inputs,
    doc_lengths,
    attn_gain,
    w_query,
    w_key,
    value_weight,
    w_output,
    mlp_gain,
    w_gate,
    w_up,
    w_down,
    out_grad,
):
    tensor_rank = lax.axis_index("tensor")
    own_rows = inputs.shape[0]
    total_rows = own_rows * lax.axis_size("tensor")
    query_cols, key_cols = w_query.shape[1], w_key.shape[1]
    joint = query_cols + 2 * key_cols
    document_segment, positions, valid_rows = layout(doc_lengths[0], total_rows)
    valid_own = lax.dynamic_slice_in_dim(valid_rows, tensor_rank * own_rows, own_rows, 0)[:, None]
    cosine, sine_part = rope_tables(positions, HEAD_SIZE)
    gain_rows = attn_gain.shape[0]
    gains = sum_everywhere(
        lax.dynamic_update_slice(
            jnp.zeros((2, inputs.shape[1]), jnp.float32),
            jnp.stack([attn_gain, mlp_gain]).astype(jnp.float32),
            (0, lax.axis_index("dp") * gain_rows),
        ),
        ("dp",),
    )
    gain_one, gain_two = gains[0], gains[1]
    packed = lax.all_gather(
        row_major(jnp.concatenate([w_query, w_key, value_weight, w_output.T], axis=1)),
        "dp",
        axis=0,
        tiled=True,
    )
    full_joint = packed[:, :joint]
    full_output = packed[:, joint:]
    hidden_units = w_gate.shape[1]
    cut = max(128, hidden_units * 5 // 8 // 128 * 128)
    down_turned = w_down.T
    halves = [
        lax.all_gather(
            row_major(
                jnp.concatenate([w_gate[:, part], w_up[:, part], down_turned[:, part]], axis=1)
            ),
            "dp",
            axis=0,
            tiled=True,
        )
        for part in (slice(0, cut), slice(cut, hidden_units))
    ]

    grad_out = out_grad.astype(jnp.float32)
    head_count = query_cols // HEAD_SIZE
    kv_heads = key_cols // HEAD_SIZE
    residual = inputs.astype(jnp.float32)
    scale_one, unit_one = rms_stats(residual)
    inputs_all = gather_rows(inputs, "tensor")
    grad_mlp_all = gather_rows(narrow(grad_out * valid_own), "tensor", relative=True)
    normed_one_all = row_major(narrow(rms_stats(inputs_all.astype(jnp.float32))[1] * gain_one))
    seg_row, seg_col = document_segment[None, :], document_segment[:, None]
    joint_turned = contract(full_joint, normed_one_all, 0, 1)
    rotated, attended, log_total = attend(
        joint_turned, cosine, sine_part, seg_row, seg_col, head_count, kv_heads, QBLK
    )
    attn_out = scatter_rows(narrow(contract(attended, full_output, 0, 1)), "tensor")
    hidden = residual + valid_own * attn_out
    scale_two, unit_two = rms_stats(hidden)
    normed_two_all = gather_rows(narrow(unit_two * gain_two), "tensor", relative=True)
    normed_split, cotangent_split = split_columns(normed_two_all), split_columns(grad_mlp_all)
    normed_total = first_act = None
    weight_grads = []
    for number, weights in enumerate(halves):
        pair_cols = 2 * (weights.shape[1] // 3)
        pair_weights, down_weights = weights[:, :pair_cols], weights[:, pair_cols:]
        pair_pre = product(normed_two_all, pair_weights)
        grad_act = product(grad_mlp_all, down_weights)
        activation, grad_pair = activation_both(pair_pre, grad_act)
        if number == 1:
            normed_total = narrow(contract(grad_pair, pair_weights, 1, 1) + normed_total.astype(jnp.float32))
            grad_pair, activation, normed_total = ordered(grad_pair, activation, normed_total)
            grad_normed_two = scatter_rows(normed_total, "tensor", relative=True)
        partial = weight_sums(((normed_split, grad_pair), (cotangent_split, activation)))
        if number == 0:
            grad_pair, activation, partial = ordered(grad_pair, activation, partial)
            normed_total = narrow(contract(grad_pair, pair_weights, 1, 1))
            first_act, first_down = activation, down_weights
            normed_two_all, grad_mlp_all, normed_total = ordered(
                normed_two_all, grad_mlp_all, normed_total
            )
        weight_grads.append(sum_shards(partial))
    mlp_gain_part = jnp.sum(grad_normed_two * unit_two, axis=0)
    grad_hidden = grad_out + norm_backward(grad_normed_two, unit_two, scale_two, gain_two)
    grad_attn = narrow(grad_hidden * valid_own)
    activation, first_act, grad_attn = ordered(activation, first_act, grad_attn)
    grad_attn_all = gather_rows(grad_attn, "tensor")
    mlp_part = narrow(
        contract(first_act, first_down, 1, 1) + contract(activation, down_weights, 1, 1)
    )
    grad_attn_all, mlp_part = ordered(grad_attn_all, mlp_part)
    mlp_out = scatter_direct(mlp_part, "tensor")
    output = hidden + valid_own * mlp_out
    grad_attended = narrow(contract(full_output, grad_attn_all, 0, 1))
    joint_back = attend_back(
        rotated,
        attended,
        grad_attended,
        log_total,
        cosine,
        sine_part,
        seg_row,
        seg_col,
        head_count,
        kv_heads,
        QBLK,
    )
    tail = weight_sums(
        (
            (split_columns(normed_one_all), joint_back.T),
            (split_columns(grad_attn_all), attended.T),
        ),
    )
    tail_grad = sum_shards(tail)
    last_part = narrow(contract(joint_back, full_joint, 0, 1))
    grad_normed_one = scatter_rows(last_part, "tensor")
    attn_gain_part = jnp.sum(grad_normed_one * unit_one, axis=0)
    input_grad = grad_hidden + norm_backward(grad_normed_one, unit_one, scale_one, gain_one)
    w_gate_grad = jnp.concatenate(
        [part[:, : part.shape[1] // 3] for part in weight_grads], axis=1
    )
    w_up_grad = jnp.concatenate(
        [part[:, part.shape[1] // 3 : 2 * (part.shape[1] // 3)] for part in weight_grads], axis=1
    )
    w_down_grad = jnp.concatenate(
        [part[:, 2 * (part.shape[1] // 3) :].T for part in weight_grads], axis=0
    )
    attn_gain_part, w_gate_grad, w_up_grad, w_down_grad = ordered(
        attn_gain_part, w_gate_grad, w_up_grad, w_down_grad
    )
    gain_sums = sum_everywhere(
        jnp.stack([attn_gain_part, mlp_gain_part]), ("tensor", "dp")
    )
    gain_own = lax.dynamic_slice_in_dim(gain_sums, lax.axis_index("dp") * gain_rows, gain_rows, 1)
    return (
        output,
        input_grad,
        gain_own[0],
        tail_grad[:, :query_cols],
        tail_grad[:, query_cols : query_cols + key_cols],
        tail_grad[:, query_cols + key_cols : joint],
        tail_grad[:, joint:].T,
        gain_own[1],
        w_gate_grad,
        w_up_grad,
        w_down_grad,
    )


def solution(mesh):
    placed = (
        P(("dp", "tensor"), None),
        P("dp", None),
        P("dp"),
        P("dp", "tensor"),
        P("dp", "tensor"),
        P("dp", "tensor"),
        P("tensor", "dp"),
        P("dp"),
        P("dp", "tensor"),
        P("dp", "tensor"),
        P("tensor", "dp"),
        P(("dp", "tensor"), None),
    )
    return jax.shard_map(
        whole_block,
        mesh=mesh,
        in_specs=placed,
        out_specs=(
            P(("dp", "tensor"), None),
            P(("dp", "tensor"), None),
            P("dp"),
            P("dp", "tensor"),
            P("dp", "tensor"),
            P("dp", "tensor"),
            P("tensor", "dp"),
            P("dp"),
            P("dp", "tensor"),
            P("dp", "tensor"),
            P("tensor", "dp"),
        ),
        check_vma=False,
    )
```

```python
import functools

import jax
import jax.numpy as jnp
from jax import lax
from jax.experimental import pallas as pl
from jax.experimental.layout import Layout, with_layout_constraint
from jax.experimental.pallas import tpu as pltpu
from jax.sharding import PartitionSpec as P


HEAD_SIZE = 64
QBLK = 256


epsilon = 1e-05
rope_base = 500000.0


def layout(lengths, total_rows):
    row_index = jnp.arange(total_rows, dtype=jnp.int32)
    doc_ends = jnp.cumsum(lengths)
    passed = doc_ends[None, :] <= row_index[:, None]
    document_segment = jnp.sum(passed.astype(jnp.int32), axis=1)
    doc_start = jnp.sum(jnp.where(passed, lengths[None, :], 0), axis=1)
    positions = (row_index - doc_start).astype(jnp.float32)
    valid_rows = (document_segment < lengths.shape[0]).astype(jnp.float32)
    return (document_segment, positions, valid_rows)


def rope_tables(positions, head_dim):
    half_dim = head_dim // 2
    inverse_freq = rope_base ** (-(jnp.arange(half_dim, dtype=jnp.float32) * 2.0 / head_dim))
    angles = positions[None, :] * inverse_freq[:, None]
    return (jnp.cos(angles), jnp.sin(angles))


def rms_stats(hidden):
    scale_row = lax.rsqrt(jnp.mean(hidden * hidden, axis=-1, keepdims=True) + epsilon)
    return (scale_row, hidden * scale_row)


def norm_backward(grad_normed, unit_rows, scale_row, gain_wide):
    scaled = grad_normed * gain_wide
    return scale_row * (scaled - unit_rows * jnp.mean(scaled * unit_rows, axis=-1, keepdims=True))


def rope_rows(ref, base, cosine, sine_part):
    half = HEAD_SIZE // 2
    first = ref[pl.ds(base, half), :]
    second = ref[pl.ds(base + half, half), :]
    return first * cosine - second * sine_part, second * cosine + first * sine_part


def fill_bias(bias_ref, seg_row_ref, seg_col_ref, start, block):
    keys = start + block
    key_index = lax.broadcasted_iota(jnp.int32, (keys, block), 0)
    query_index = lax.broadcasted_iota(jnp.int32, (keys, block), 1) + start
    allowed = (seg_col_ref[:keys, :] == seg_row_ref[:, start : start + block]) & (
        key_index <= query_index
    )
    bias_ref[:keys, :] = jnp.where(allowed, 0.0, -jnp.inf)


def head_base(index):
    return pl.multiple_of(index * HEAD_SIZE, HEAD_SIZE)


def turned(value):
    return jnp.transpose(value.astype(jnp.float32)).astype(jnp.bfloat16)


def attend_kernel(
    heads, kv_heads, block, joint_ref, cos_ref, sin_ref, seg_row_ref, seg_col_ref,
    rot_ref, att_ref, log_ref, krow_ref, bias_ref,
):
    rows = joint_ref.shape[1]
    half = HEAD_SIZE // 2
    group = heads // kv_heads
    value_base = (heads + kv_heads) * HEAD_SIZE

    def rotate_head(index, scale):
        base = head_base(index)
        first, second = rope_rows(joint_ref, base, cos_ref[...], sin_ref[...])
        rot_ref[pl.ds(base, half), :] = (first * scale).astype(jnp.bfloat16)
        rot_ref[pl.ds(base + half, half), :] = (second * scale).astype(jnp.bfloat16)

    @pl.loop(0, heads)
    def _(index):
        rotate_head(index, HEAD_SIZE ** (-0.5))

    @pl.loop(0, kv_heads)
    def _(index):
        rotate_head(heads + index, 1.0)
        krow_ref[index] = turned(rot_ref[pl.ds(head_base(heads + index), HEAD_SIZE), :])

    rot_ref[value_base:, :] = joint_ref[value_base:, :].astype(jnp.bfloat16)
    for start in range(0, rows, block):
        keys = start + block
        fill_bias(bias_ref, seg_row_ref, seg_col_ref, start, block)

        @pl.loop(0, heads)
        def _(head):
            kv_head = head // group
            query = rot_ref[pl.ds(head_base(head), HEAD_SIZE), start:keys]
            scores = (
                jnp.dot(krow_ref[kv_head, :keys, :], query, preferred_element_type=jnp.float32)
                + bias_ref[:keys, :]
            )
            top = jnp.max(scores, axis=0, keepdims=True)
            powers = jnp.exp(scores - top)
            total = jnp.sum(powers, axis=0, keepdims=True)
            weights = (powers * (1.0 / total)).astype(jnp.bfloat16)
            value = rot_ref[pl.ds(head_base(heads + kv_heads + kv_head), HEAD_SIZE), :keys]
            att_ref[pl.ds(head_base(head), HEAD_SIZE), start:keys] = jnp.dot(
                value, weights, preferred_element_type=jnp.float32
            ).astype(jnp.bfloat16)
            log_ref[pl.ds(head, 1), start:keys] = top + jnp.log(total)


def attend_back_kernel(
    heads, kv_heads, block, rot_ref, att_ref, out_ref, log_ref, cos_ref, sin_ref,
    seg_row_ref, seg_col_ref, back_ref, krow_ref, vrow_ref, dkey_ref, dvalue_ref, bias_ref,
):
    rows = rot_ref.shape[1]
    half = HEAD_SIZE // 2
    group = heads // kv_heads
    last = (((1,), (1,)), ((), ()))

    def turn_back(first, second, base, start, stop):
        cosine, sine_part = cos_ref[:, start:stop], sin_ref[:, start:stop]
        back_ref[pl.ds(base, half), start:stop] = (
            first * cosine + second * sine_part
        ).astype(jnp.bfloat16)
        back_ref[pl.ds(base + half, half), start:stop] = (
            second * cosine - first * sine_part
        ).astype(jnp.bfloat16)

    @pl.loop(0, kv_heads)
    def _(index):
        krow_ref[index] = turned(rot_ref[pl.ds(head_base(heads + index), HEAD_SIZE), :])
        vrow_ref[index] = turned(rot_ref[pl.ds(head_base(heads + kv_heads + index), HEAD_SIZE), :])

    dkey_ref[...] = jnp.zeros_like(dkey_ref)
    dvalue_ref[...] = jnp.zeros_like(dvalue_ref)
    for start in range(0, rows, block):
        keys = start + block
        fill_bias(bias_ref, seg_row_ref, seg_col_ref, start, block)

        @pl.loop(0, heads)
        def _(head):
            kv_head = head // group
            own = pl.ds(head_base(head), HEAD_SIZE)
            query = rot_ref[own, start:keys]
            grad = out_ref[own, start:keys]
            delta = jnp.sum(
                grad.astype(jnp.float32) * att_ref[own, start:keys].astype(jnp.float32),
                axis=0,
                keepdims=True,
            )
            scores = (
                jnp.dot(krow_ref[kv_head, :keys, :], query, preferred_element_type=jnp.float32)
                + bias_ref[:keys, :]
            )
            probs = jnp.exp(scores - log_ref[pl.ds(head, 1), start:keys])
            grad_probs = jnp.dot(
                vrow_ref[kv_head, :keys, :], grad, preferred_element_type=jnp.float32
            )
            grad_scores = (probs * (grad_probs - delta)).astype(jnp.bfloat16)
            dvalue_ref[kv_head, :keys, :] += lax.dot_general(
                probs.astype(jnp.bfloat16), grad, last, preferred_element_type=jnp.float32
            )
            dkey_ref[kv_head, :keys, :] += lax.dot_general(
                grad_scores, query, last, preferred_element_type=jnp.float32
            )
            key = rot_ref[pl.ds(head_base(heads + kv_head), HEAD_SIZE), :keys]
            dquery = jnp.dot(key, grad_scores, preferred_element_type=jnp.float32) * (
                HEAD_SIZE ** (-0.5)
            )
            turn_back(dquery[:half], dquery[half:], head_base(head), start, keys)

    @pl.loop(0, kv_heads)
    def _(index):
        dkey = jnp.transpose(dkey_ref[index])
        turn_back(dkey[:half], dkey[half:], head_base(heads + index), 0, rows)
        back_ref[pl.ds(head_base(heads + kv_heads + index), HEAD_SIZE), :] = jnp.transpose(
            dvalue_ref[index]
        ).astype(jnp.bfloat16)


def activation_kernel(pair_ref, grad_ref, act_ref, out_ref):
    units = grad_ref.shape[1]
    gate, up = pair_ref[:, :units], pair_ref[:, units:]
    grad = grad_ref[...]
    sigmoid_gate = 1.0 / (1.0 + jnp.exp(-gate))
    act_ref[...] = (gate * sigmoid_gate * up).astype(jnp.bfloat16)
    grad_gate = grad * up * sigmoid_gate * (1.0 + gate * (1.0 - sigmoid_gate))
    out_ref[:, :units] = grad_gate.astype(jnp.bfloat16)
    out_ref[:, units:] = (grad * gate * sigmoid_gate).astype(jnp.bfloat16)


def activation_both(pair, grad):
    rows, units = grad.shape
    block = min(rows, 256)

    def at(row):
        return (row, 0)

    return pl.pallas_call(
        activation_kernel,
        out_shape=(
            jax.ShapeDtypeStruct(grad.shape, jnp.bfloat16),
            jax.ShapeDtypeStruct(pair.shape, jnp.bfloat16),
        ),
        grid=(rows // block,),
        in_specs=[pl.BlockSpec((block, 2 * units), at), pl.BlockSpec((block, units), at)],
        out_specs=(pl.BlockSpec((block, units), at), pl.BlockSpec((block, 2 * units), at)),
        cost_estimate=pl.CostEstimate(
            flops=20 * pair.size, bytes_accessed=9 * pair.size, transcendentals=pair.size
        ),
        name="activation_both",
    )(pair, grad)


def in_vmem(count):
    return [pl.BlockSpec(memory_space=pltpu.VMEM)] * count


def attend(joint, cosine, sine_part, seg_row, seg_col, heads, kv_heads, block):
    rows = joint.shape[1]
    flops = 2 * heads * rows * rows * HEAD_SIZE
    return pl.pallas_call(
        functools.partial(attend_kernel, heads, kv_heads, block),
        out_shape=(
            jax.ShapeDtypeStruct(joint.shape, jnp.bfloat16),
            jax.ShapeDtypeStruct((heads * HEAD_SIZE, rows), jnp.bfloat16),
            jax.ShapeDtypeStruct((heads, rows), jnp.float32),
        ),
        in_specs=in_vmem(5),
        out_specs=tuple(in_vmem(3)),
        scratch_shapes=[
            pltpu.VMEM((kv_heads, rows, HEAD_SIZE), jnp.bfloat16),
            pltpu.VMEM((rows, block), jnp.float32),
        ],
        cost_estimate=pl.CostEstimate(
            flops=8 * flops, bytes_accessed=8 * joint.size, transcendentals=heads * rows * rows
        ),
        name="attend",
    )(joint, cosine, sine_part, seg_row, seg_col)


def attend_back(rotated, attended, grad, log_total, cosine, sine_part, seg_row, seg_col, heads, kv_heads, block):
    rows = rotated.shape[1]
    flops = 2 * heads * rows * rows * HEAD_SIZE
    return pl.pallas_call(
        functools.partial(attend_back_kernel, heads, kv_heads, block),
        out_shape=jax.ShapeDtypeStruct(rotated.shape, jnp.bfloat16),
        in_specs=in_vmem(8),
        out_specs=pl.BlockSpec(memory_space=pltpu.VMEM),
        scratch_shapes=[
            pltpu.VMEM((kv_heads, rows, HEAD_SIZE), jnp.bfloat16),
            pltpu.VMEM((kv_heads, rows, HEAD_SIZE), jnp.bfloat16),
            pltpu.VMEM((kv_heads, rows, HEAD_SIZE), jnp.float32),
            pltpu.VMEM((kv_heads, rows, HEAD_SIZE), jnp.float32),
            pltpu.VMEM((rows, block), jnp.float32),
        ],
        cost_estimate=pl.CostEstimate(
            flops=20 * flops, bytes_accessed=8 * rotated.size, transcendentals=heads * rows * rows
        ),
        name="attend_back",
    )(rotated, attended, grad, log_total, cosine, sine_part, seg_row, seg_col)


def shift_pairs(count, mask):
    return [(i, i ^ mask) for i in range(count)]


def gather_rows(block, axis, relative=False):
    count = lax.axis_size(axis)
    if count != 4:
        return lax.all_gather(block, axis, axis=0, tiled=True)
    me = lax.axis_index(axis)
    rows = block.shape[0]
    half = rows // 2
    from_x = lax.ppermute(block, axis, shift_pairs(count, 1))
    from_y = lax.ppermute(block, axis, shift_pairs(count, 2))
    far_top = lax.ppermute(from_x[:half], axis, shift_pairs(count, 2))
    far_low = lax.ppermute(from_y[half:], axis, shift_pairs(count, 1))
    if relative:
        return jnp.concatenate([block, from_x, from_y, far_top, far_low], axis=0)
    whole = jnp.zeros((count * rows, block.shape[1]), block.dtype)
    for mask, piece, extra in (
        (0, block, 0),
        (1, from_x, 0),
        (2, from_y, 0),
        (3, far_top, 0),
        (3, far_low, half),
    ):
        whole = lax.dynamic_update_slice(whole, piece, ((me ^ mask) * rows + extra, 0))
    return row_major(whole)


def scatter_rows(partial, axis, relative=False):
    count = lax.axis_size(axis)
    if count != 4:
        return lax.psum_scatter(partial, axis, scatter_dimension=0, tiled=True).astype(jnp.float32)
    me = 0 if relative else lax.axis_index(axis)
    rows = partial.shape[0] // count
    half = rows // 2

    def part(mask, extra):
        return lax.dynamic_slice_in_dim(partial, (me ^ mask) * rows + extra, half, 0)

    def send(piece, mask):
        return lax.ppermute(piece, axis, shift_pairs(count, mask))

    relay_top = send(part(3, 0), 1).astype(jnp.float32)
    relay_low = send(part(3, half), 2).astype(jnp.float32)
    near_top = send(part(1, 0), 1).astype(jnp.float32)
    near_low = send(part(2, half), 2).astype(jnp.float32)
    top_sum, low_sum = ordered(narrow(part(2, 0) + relay_top), narrow(part(1, half) + relay_low))
    joined_top = send(top_sum, 2).astype(jnp.float32)
    joined_low = send(low_sum, 1).astype(jnp.float32)
    return jnp.concatenate(
        [part(0, 0) + near_top + joined_top, part(0, half) + near_low + joined_low], axis=0
    )


def scatter_direct(partial, axis):
    count = lax.axis_size(axis)
    if count != 4:
        return lax.psum_scatter(partial, axis, scatter_dimension=0, tiled=True).astype(jnp.float32)
    rows = partial.shape[0] // count
    total = partial[:rows].astype(jnp.float32)
    for mask in (3, 1, 2):
        piece = partial[mask * rows : (mask + 1) * rows]
        got = lax.ppermute(piece, axis, shift_pairs(count, mask))
        total = total + got.astype(jnp.float32)
    return total


def paired():
    count = lax.axis_size("dp")
    return count > 2 and count % 2 == 0


def line_gather(block):
    if not paired():
        return lax.all_gather(block, "dp", axis=0, tiled=True)
    count = lax.axis_size("dp")
    lines = count // 2
    line, core = lax.axis_index("dp") // 2, lax.axis_index("dp") % 2
    rows, width = block.shape
    lower, upper = [], []
    low = high = block
    for step in range(lines - 1):
        low = lax.ppermute(low, "dp", [(i, i + 2) for i in range(2 * step, count - 2)])
        high = lax.ppermute(high, "dp", [(i, i - 2) for i in range(2, count - 2 * step)])
        lower.append(low)
        upper.append(high)
    around = jnp.concatenate(lower[::-1] + [block] + upper, axis=0)
    mine = lax.dynamic_slice_in_dim(around, (lines - 1 - line) * rows, lines * rows, 0)
    other = lax.ppermute(mine, "dp", shift_pairs(count, 1))
    mine, other = mine.reshape(lines, 1, rows, width), other.reshape(lines, 1, rows, width)
    even, odd = jnp.where(core == 0, mine, other), jnp.where(core == 0, other, mine)
    return row_major(jnp.concatenate([even, odd], axis=1).reshape(count * rows, width))


def row_major(value):
    return with_layout_constraint(value, Layout(major_to_minor=(0, 1)))


def split_columns(rows):
    count = lax.axis_size("dp")
    if not paired():
        return rows, None
    width = rows.shape[1] // count
    core = lax.axis_index("dp") % 2

    def half(which):
        return row_major(
            jnp.concatenate(
                [
                    lax.dynamic_slice_in_dim(rows, (first + which) * width, width, 1)
                    for first in range(0, count, 2)
                ],
                axis=1,
            )
        )

    return half(core), half(1 - core)


def weight_sums(pairs):
    keeps = []
    for (keep_rows, send_rows), right in pairs:
        if send_rows is None:
            keeps.append(narrow(contract(keep_rows, right, 0, 0)))
            continue
        sent = narrow(contract(send_rows, right, 0, 0))
        count = lax.axis_size("dp")
        got = lax.ppermute(sent, "dp", shift_pairs(count, 1))
        keeps.append(narrow(contract(keep_rows, right, 0, 0) + got.astype(jnp.float32)))
    return row_major(jnp.concatenate(keeps, axis=1))


def sum_shards(partial):
    count = lax.axis_size("dp")
    groups = [list(range(core, count, 2)) for core in range(2)] if paired() else None
    summed = lax.psum_scatter(
        partial, "dp", scatter_dimension=0, tiled=True, axis_index_groups=groups
    )
    return summed.astype(jnp.float32)


def sum_everywhere(value, axes):
    for axis in axes:
        count = lax.axis_size(axis)
        if count & (count - 1):
            value = lax.psum(value, axis)
            continue
        step = 1
        while step < count:
            value = value + lax.ppermute(value, axis, shift_pairs(count, step))
            step *= 2
    return value


def product(left, right):
    return jnp.dot(left, right, preferred_element_type=jnp.float32)


def contract(left, right, left_axis, right_axis):
    return lax.dot_general(
        left,
        right,
        (((left_axis,), (right_axis,)), ((), ())),
        preferred_element_type=jnp.float32,
    )


def ordered(*values):
    return lax.optimization_barrier(values)


def narrow(value):
    return value.astype(jnp.bfloat16)


def whole_block(
    inputs,
    doc_lengths,
    attn_gain,
    w_query,
    w_key,
    value_weight,
    w_output,
    mlp_gain,
    w_gate,
    w_up,
    w_down,
    out_grad,
):
    tensor_rank = lax.axis_index("tensor")
    own_rows = inputs.shape[0]
    total_rows = own_rows * lax.axis_size("tensor")
    query_cols, key_cols = w_query.shape[1], w_key.shape[1]
    joint = query_cols + 2 * key_cols
    document_segment, positions, valid_rows = layout(doc_lengths[0], total_rows)
    valid_own = lax.dynamic_slice_in_dim(valid_rows, tensor_rank * own_rows, own_rows, 0)[:, None]
    cosine, sine_part = rope_tables(positions, HEAD_SIZE)
    gain_rows = attn_gain.shape[0]
    gains = sum_everywhere(
        lax.dynamic_update_slice(
            jnp.zeros((2, inputs.shape[1]), jnp.float32),
            jnp.stack([attn_gain, mlp_gain]).astype(jnp.float32),
            (0, lax.axis_index("dp") * gain_rows),
        ),
        ("dp",),
    )
    gain_one, gain_two = gains[0], gains[1]
    packed = lax.all_gather(
        row_major(jnp.concatenate([w_query, w_key, value_weight, w_output.T], axis=1)),
        "dp",
        axis=0,
        tiled=True,
    )
    full_joint = packed[:, :joint]
    full_output = packed[:, joint:]
    hidden_units = w_gate.shape[1]
    cut = max(128, hidden_units * 5 // 8 // 128 * 128)
    down_turned = w_down.T
    first, second = slice(0, cut), slice(cut, hidden_units)
    halves = [
        lax.all_gather(row_major(jnp.concatenate(parts, axis=1)), "dp", axis=0, tiled=True)
        for parts in (
            [w_gate[:, first], w_up[:, first], down_turned[:, first]],
            [w_gate[:, second], w_up[:, second]],
        )
    ]
    last_down = line_gather(row_major(down_turned[:, second]))
    halves = [
        (halves[0][:, : 2 * cut], halves[0][:, 2 * cut :]),
        (halves[1], last_down),
    ]

    grad_out = out_grad.astype(jnp.float32)
    head_count = query_cols // HEAD_SIZE
    kv_heads = key_cols // HEAD_SIZE
    residual = inputs.astype(jnp.float32)
    scale_one, unit_one = rms_stats(residual)
    inputs_all = gather_rows(inputs, "tensor")
    grad_mlp_all = gather_rows(narrow(grad_out * valid_own), "tensor", relative=True)
    normed_one_all = row_major(narrow(rms_stats(inputs_all.astype(jnp.float32))[1] * gain_one))
    seg_row, seg_col = document_segment[None, :], document_segment[:, None]
    joint_turned = contract(full_joint, normed_one_all, 0, 1)
    rotated, attended, log_total = attend(
        joint_turned, cosine, sine_part, seg_row, seg_col, head_count, kv_heads, QBLK
    )
    attn_out = scatter_rows(narrow(contract(attended, full_output, 0, 1)), "tensor")
    hidden = residual + valid_own * attn_out
    scale_two, unit_two = rms_stats(hidden)
    normed_two_all = gather_rows(narrow(unit_two * gain_two), "tensor", relative=True)
    normed_split, cotangent_split = split_columns(normed_two_all), split_columns(grad_mlp_all)
    normed_total = first_act = None
    weight_grads = []
    for number, weights in enumerate(halves):
        pair_weights, down_weights = weights
        pair_pre = product(normed_two_all, pair_weights)
        grad_act = product(grad_mlp_all, down_weights)
        activation, grad_pair = activation_both(pair_pre, grad_act)
        if number == 1:
            normed_total = narrow(contract(grad_pair, pair_weights, 1, 1) + normed_total.astype(jnp.float32))
            grad_pair, activation, normed_total = ordered(grad_pair, activation, normed_total)
            grad_normed_two = scatter_rows(normed_total, "tensor", relative=True)
        partial = weight_sums(((normed_split, grad_pair), (cotangent_split, activation)))
        if number == 0:
            grad_pair, activation, partial = ordered(grad_pair, activation, partial)
            normed_total = narrow(contract(grad_pair, pair_weights, 1, 1))
            first_act, first_down = activation, down_weights
            normed_two_all, grad_mlp_all, normed_total = ordered(
                normed_two_all, grad_mlp_all, normed_total
            )
        weight_grads.append(sum_shards(partial))
    mlp_gain_part = jnp.sum(grad_normed_two * unit_two, axis=0)
    grad_hidden = grad_out + norm_backward(grad_normed_two, unit_two, scale_two, gain_two)
    grad_attn = narrow(grad_hidden * valid_own)
    activation, first_act, grad_attn = ordered(activation, first_act, grad_attn)
    grad_attn_all = gather_rows(grad_attn, "tensor")
    mlp_part = narrow(
        contract(first_act, first_down, 1, 1) + contract(activation, down_weights, 1, 1)
    )
    grad_attn_all, mlp_part = ordered(grad_attn_all, mlp_part)
    mlp_out = scatter_direct(mlp_part, "tensor")
    output = hidden + valid_own * mlp_out
    grad_attended = narrow(contract(full_output, grad_attn_all, 0, 1))
    joint_back = attend_back(
        rotated,
        attended,
        grad_attended,
        log_total,
        cosine,
        sine_part,
        seg_row,
        seg_col,
        head_count,
        kv_heads,
        QBLK,
    )
    tail = weight_sums(
        (
            (split_columns(normed_one_all), joint_back.T),
            (split_columns(grad_attn_all), attended.T),
        ),
    )
    tail_grad = sum_shards(tail)
    last_part = narrow(contract(joint_back, full_joint, 0, 1))
    grad_normed_one = scatter_rows(last_part, "tensor")
    attn_gain_part = jnp.sum(grad_normed_one * unit_one, axis=0)
    input_grad = grad_hidden + norm_backward(grad_normed_one, unit_one, scale_one, gain_one)
    w_gate_grad = jnp.concatenate(
        [part[:, : part.shape[1] // 3] for part in weight_grads], axis=1
    )
    w_up_grad = jnp.concatenate(
        [part[:, part.shape[1] // 3 : 2 * (part.shape[1] // 3)] for part in weight_grads], axis=1
    )
    w_down_grad = jnp.concatenate(
        [part[:, 2 * (part.shape[1] // 3) :].T for part in weight_grads], axis=0
    )
    attn_gain_part, w_gate_grad, w_up_grad, w_down_grad = ordered(
        attn_gain_part, w_gate_grad, w_up_grad, w_down_grad
    )
    gain_sums = sum_everywhere(
        jnp.stack([attn_gain_part, mlp_gain_part]), ("tensor", "dp")
    )
    gain_own = lax.dynamic_slice_in_dim(gain_sums, lax.axis_index("dp") * gain_rows, gain_rows, 1)
    return (
        output,
        input_grad,
        gain_own[0],
        tail_grad[:, :query_cols],
        tail_grad[:, query_cols : query_cols + key_cols],
        tail_grad[:, query_cols + key_cols : joint],
        tail_grad[:, joint:].T,
        gain_own[1],
        w_gate_grad,
        w_up_grad,
        w_down_grad,
    )


def solution(mesh):
    placed = (
        P(("dp", "tensor"), None),
        P("dp", None),
        P("dp"),
        P("dp", "tensor"),
        P("dp", "tensor"),
        P("dp", "tensor"),
        P("tensor", "dp"),
        P("dp"),
        P("dp", "tensor"),
        P("dp", "tensor"),
        P("tensor", "dp"),
        P(("dp", "tensor"), None),
    )
    return jax.shard_map(
        whole_block,
        mesh=mesh,
        in_specs=placed,
        out_specs=(
            P(("dp", "tensor"), None),
            P(("dp", "tensor"), None),
            P("dp"),
            P("dp", "tensor"),
            P("dp", "tensor"),
            P("dp", "tensor"),
            P("tensor", "dp"),
            P("dp"),
            P("dp", "tensor"),
            P("dp", "tensor"),
            P("tensor", "dp"),
        ),
        check_vma=False,
    )
```
